32 devices in a mesh: dp: 8 (over z, y), mp: 4 (over x, core).
Axes of the slice: x: 2, y: 2, z: 4, core: 2. Of those that a mesh axis runs over, the one named last changes fastest.
Arguments:
- queries: bfloat16 [24576, 2048], P('dp', 'mp'), may hold values from -30 to 30
- keys: bfloat16 [24576, 512], P('dp', 'mp'), may hold values from -30 to 30
- values: bfloat16 [24576, 512], P('dp', 'mp'), may hold values from -6 to 6
- doc_ids: int32 [24576], P('dp'), may hold values from -1 to 127, as said below
- live_counts: int32 [8], P('dp'), may hold values from 1 to 24, 176 in all
- out_weight: bfloat16 [2048, 4096], P('dp', 'mp'), may hold values from -0.125 to 0.125
Outputs:
- mixed: bfloat16 [22528, 4096], P('dp', 'mp')
The draws below stay inside these ranges and needn't reach their ends.
Inputs may be any that keep to these rules, and one draw needn't show every extreme that they name: `live_counts`: each device has 1 to 24 live blocks, 176 in all, and some device has exactly 24. `doc_ids`: within each block the numbers start at 0 and never fall along the block, and the -1 entries, if any, form the block's tail.
All inputs are finite; a program needn't handle non-finite values.
Results may differ from the reference program's by a relative error of at most 0.0049.
Values may be sent and summed in bfloat16 or wider, within the bound.
A program may use at most 128 MiB of HBM per device.

```python
import math
import jax
import jax.numpy as jnp
import numpy as np
from jax import lax

D = 4096
HEAD_SIZE = 128
HQ = 16
KEY_VALUE_HEADS = 4
BLOCK = 128
NB = 24
RCAP = 22
TOKEN_POSITIONS = 24576
N_DP = 8


def draw_queries(key, part):
    drawn_result = jnp.clip(jax.random.normal(jax.random.fold_in(key, 1), (TOKEN_POSITIONS, HQ * HEAD_SIZE), jnp.float32), -6.0, 6.0)
    return drawn_result.astype(jnp.bfloat16)


def draw_keys(key, part):
    drawn_result = jnp.clip(jax.random.normal(jax.random.fold_in(key, 2), (TOKEN_POSITIONS, KEY_VALUE_HEADS * HEAD_SIZE), jnp.float32), -6.0, 6.0)
    return drawn_result.astype(jnp.bfloat16)


def draw_doc_ids(key, part):
    blocks = TOKEN_POSITIONS // BLOCK
    places = jnp.arange(BLOCK, dtype=jnp.int32)[None, :]
    cuts = jax.random.randint(jax.random.fold_in(key, 21), (blocks, BLOCK), 0, 24) == 0
    cuts = cuts & (places > 0)
    numbers = jnp.cumsum(cuts.astype(jnp.int32), axis=1).astype(jnp.int32)
    filled = jax.random.randint(jax.random.fold_in(key, 22), (blocks, 1), BLOCK // 2, BLOCK + 1)
    numbers = jnp.where(places < filled, numbers, -1)
    first_block = jnp.arange(blocks, dtype=jnp.int32)[:, None] == 0
    numbers = jnp.where(first_block, places, numbers)
    return numbers.reshape(TOKEN_POSITIONS).astype(jnp.int32)


def levels(own_key, dims, shards, least, largest):
    factor_of, own = 1.0, jax.random.fold_in(own_key, 6)
    for axis_at, shards_of in shards:
        heights = jnp.exp(jax.random.uniform(jax.random.fold_in(own, axis_at), (shards_of,), jnp.float32, least / len(shards), largest / len(shards)))
        factor_of = factor_of * jnp.repeat(heights, dims[axis_at] // shards_of).reshape([-1 if axis == axis_at else 1 for axis in range(len(dims))])
    return factor_of


def profile(count, total, most, skew):
    loads = [(1 << 20) // math.isqrt(standing ** skew) + 1 for standing in range(2, count + 1)]
    rest, counts = total - most - (count - 1), [1] * (count - 1)
    while rest > 0:
        free = [i for i in range(count - 1) if counts[i] < most]
        whole, remaining = sum([loads[i] for i in free]), rest
        for i in free:
            more = min(most - counts[i], max(1, remaining * loads[i] // whole), rest)
            counts[i] = counts[i] + more
            rest = rest - more
    return np.array([most] + counts)


def uneven(rng, amount, total, bound, skew):
    if amount == 2:
        one = jax.random.randint(rng, (), max(1, total - bound), min(bound, total - 1) + 1)
        return jnp.stack([one, total - one])
    lengths = jnp.asarray(profile(amount, total, bound, skew), jnp.int32)
    pairs = (amount - 1) // 2
    donor, sink = lengths[1:1 + 2 * pairs:2], lengths[2:2 + 2 * pairs:2]
    room = jnp.minimum(donor - 1, bound - sink)
    shifted = jax.random.randint(jax.random.fold_in(rng, 1), (pairs,), 0, 1 << 20) % (room + 1)
    lengths = lengths.at[1:1 + 2 * pairs:2].set(donor - shifted).at[2:2 + 2 * pairs:2].set(sink + shifted)
    return lengths[jax.random.permutation(jax.random.fold_in(rng, 2), amount)]


def gaussian(key, dims, spread, limit, shards=(), held_as=jnp.bfloat16):
    level = levels(key, dims, shards, -0.22, 0.18) if shards else 1.0
    values = jax.random.normal(key, dims, jnp.float32) * spread * level
    return jnp.minimum(jnp.maximum(values, -limit), limit).astype(held_as)


def setup_inputs(seed: int = 0) -> dict:
    key_of = jax.random.split(jax.random.key(seed), 7)
    return {
        "queries": draw_queries(jax.random.fold_in(key_of[6], 71), 0),
        "keys": draw_keys(jax.random.fold_in(key_of[6], 71), 0),
        "values": gaussian(key_of[2], (TOKEN_POSITIONS, KEY_VALUE_HEADS * HEAD_SIZE), 1.0, 6.0, ((0, 8), (1, 4))),
        "doc_ids": draw_doc_ids(jax.random.fold_in(key_of[6], 71), 0),
        "live_counts": uneven(key_of[4], N_DP, N_DP * RCAP, NB, 2).astype(jnp.int32),
        "out_weight": gaussian(key_of[5], (HQ * HEAD_SIZE, D), (HQ * HEAD_SIZE) ** -0.5, 0.125, ((0, 8), (1, 4))),
    }


masked_score = -1e+30

def attend_blocks(query_blocks, key_blocks, value_blocks, id_blocks):
    number = query_blocks.shape[0]
    query_heads = query_blocks.shape[2] // HEAD_SIZE
    key_heads = key_blocks.shape[2] // HEAD_SIZE
    repeat = query_heads // key_heads
    query_four = query_blocks.astype(jnp.float32).reshape(number, BLOCK, key_heads, repeat, HEAD_SIZE)
    key_four = key_blocks.astype(jnp.float32).reshape(number, BLOCK, key_heads, HEAD_SIZE)
    value_four = value_blocks.astype(jnp.float32).reshape(number, BLOCK, key_heads, HEAD_SIZE)
    scores = jnp.einsum('bihrd,bjhd->bhrij', query_four, key_four) / math.sqrt(HEAD_SIZE)
    places = jnp.arange(BLOCK, dtype=jnp.int32)
    causal = places[None, :] <= places[:, None]
    allowed = (id_blocks[:, :, None] == id_blocks[:, None, :]) & causal[None]
    scores = jnp.where(allowed[:, None, None], scores, masked_score)
    highest = lax.optimization_barrier(jnp.max(scores, axis=-1, keepdims=True))
    weights = jnp.where(allowed[:, None, None], jnp.exp(scores - highest), 0.0)
    total_counts = lax.optimization_barrier(jnp.sum(weights, axis=-1))
    rounded_counts = lax.optimization_barrier(weights.astype(jnp.bfloat16)).astype(jnp.float32)
    summed = jnp.einsum('bhrij,bjhd->bihrd', rounded_counts, value_four)
    summed = summed / jnp.transpose(total_counts, (0, 3, 1, 2))[..., None]
    summed = jnp.where(id_blocks[:, :, None, None, None] >= 0, summed, 0.0)
    return summed.reshape(number, BLOCK, query_heads * HEAD_SIZE).astype(jnp.bfloat16)

def reference(queries, keys, values, doc_ids, live_counts, out_weight):
    inclusive = jnp.cumsum(live_counts).astype(jnp.int32)
    exclusive = inclusive - live_counts
    owners = jnp.arange(N_DP, dtype=jnp.int32)[:, None]
    places = jnp.arange(RCAP, dtype=jnp.int32)[None, :]
    labels = (places * N_DP + owners).reshape(-1)
    holder = lax.optimization_barrier(jnp.sum((inclusive[None, :] <= labels[:, None]).astype(jnp.int32), axis=1))
    within = labels - exclusive[holder]
    chosen = (holder * NB + within).astype(jnp.int32)
    query_blocks = queries.reshape(N_DP * NB, BLOCK, -1)[chosen]
    key_blocks = keys.reshape(N_DP * NB, BLOCK, -1)[chosen]
    value_blocks = values.reshape(N_DP * NB, BLOCK, -1)[chosen]
    id_blocks = doc_ids.reshape(N_DP * NB, BLOCK)[chosen]

    def owner_rows(operands):
        attended = attend_blocks(operands[0], operands[1], operands[2], operands[3])
        flattened = attended.reshape(RCAP * BLOCK, HQ * HEAD_SIZE)
        return jnp.dot(flattened, out_weight, preferred_element_type=jnp.float32).astype(jnp.bfloat16)
    stacked = lax.map(owner_rows, (query_blocks.reshape(N_DP, RCAP, BLOCK, -1), key_blocks.reshape(N_DP, RCAP, BLOCK, -1), value_blocks.reshape(N_DP, RCAP, BLOCK, -1), id_blocks.reshape(N_DP, RCAP, BLOCK)))
    return stacked.reshape(N_DP * RCAP * BLOCK, D)
```

```python
import functools
import math

import jax
import jax.numpy as jnp
from jax import lax
from jax.experimental import pallas as pl
from jax.experimental.pallas import tpu as pltpu
from jax.sharding import PartitionSpec as P

HEAD_SIZE = 128
BLOCK = 128
NB = 24
MESH = pl.DeviceIdType.MESH
MASKED = -1e30
VMEM = 60 * 1024 * 1024


def attend_kernel(per_owner, plan_ref, queries_ref, keys_ref, values_ref, ids_ref, out_ref):
    step = pl.program_id(0)
    repeat = queries_ref.shape[1] // HEAD_SIZE
    factor = math.log2(math.e) / math.sqrt(HEAD_SIZE)
    row_at = lax.broadcasted_iota(jnp.int32, (BLOCK, BLOCK), 0)
    col_at = lax.broadcasted_iota(jnp.int32, (BLOCK, BLOCK), 1)
    causal = col_at <= row_at
    ones = jnp.ones((BLOCK, HEAD_SIZE), jnp.bfloat16)
    for layer in range(per_owner):
        block = plan_ref[0, step * per_owner + layer]
        rows = pl.ds(pl.multiple_of(block * BLOCK, BLOCK), BLOCK)
        along = jnp.broadcast_to(ids_ref[pl.ds(block, 1), :], (BLOCK, BLOCK))
        down = along.T
        bias = jnp.where((along == down) & causal, 0.0, MASKED)
        value = jnp.where(down >= 0, values_ref[rows, :].astype(jnp.float32), 0.0)
        value = jnp.concatenate([value.astype(jnp.bfloat16), ones], axis=1)
        key = keys_ref[rows, :]
        query = queries_ref[rows, :]
        query = jnp.concatenate(
            [query[:, h * HEAD_SIZE:(h + 1) * HEAD_SIZE] for h in range(repeat)], axis=0
        )
        scores = lax.dot_general(
            query, key, (((1,), (1,)), ((), ())), preferred_element_type=jnp.float32
        )
        weights = []
        for head in range(repeat):
            part = scores[head * BLOCK:(head + 1) * BLOCK] + bias
            highest = jnp.max(part, axis=1, keepdims=True)
            weights.append(jnp.exp2((part - highest) * factor).astype(jnp.bfloat16))
        summed = jnp.dot(
            jnp.concatenate(weights, axis=0), value, preferred_element_type=jnp.float32
        )
        summed = summed[:, :HEAD_SIZE] / summed[:, HEAD_SIZE:]
        for head in range(repeat):
            columns = slice(head * HEAD_SIZE, (head + 1) * HEAD_SIZE)
            out_ref[0, layer, :, columns] = summed[head * BLOCK:(head + 1) * BLOCK].astype(
                out_ref.dtype
            )


def attend(plan, queries, keys, values, ids, members, per_owner):
    cols = queries.shape[1]

    def whole(array):
        return pl.BlockSpec(array.shape, lambda i, c: (0, 0))

    return pl.pallas_call(
        functools.partial(attend_kernel, per_owner),
        out_shape=jax.ShapeDtypeStruct((members, per_owner, BLOCK, cols), jnp.bfloat16),
        grid_spec=pltpu.PrefetchScalarGridSpec(
            num_scalar_prefetch=1,
            grid=(members,),
            in_specs=[whole(queries), whole(keys), whole(values), whole(ids)],
            out_specs=pl.BlockSpec((1, per_owner, BLOCK, cols), lambda i, c: (i, 0, 0, 0)),
        ),
        compiler_params=pltpu.CompilerParams(vmem_limit_bytes=VMEM),
        cost_estimate=pl.CostEstimate(
            flops=members * per_owner * cols * BLOCK * BLOCK * 4,
            bytes_accessed=4 * queries.size,
            transcendentals=members * per_owner * cols * BLOCK,
        ),
    )(plan, queries, keys, values, ids)


def flip(index, mask):
    bit = 1
    while bit <= mask:
        if mask & bit:
            index = index + bit - 2 * bit * ((index // bit) % 2)
        bit *= 2
    return index


def plan_kernel(members, per_owner, count_ref, plan_ref, table_ref, send_sem, recv_sem):
    me = lax.axis_index("dp")
    mine = lax.axis_index("mp")
    barrier = pltpu.get_barrier_semaphore()
    for mask in range(1, members):
        pl.semaphore_signal(
            barrier, inc=1, device_id=(flip(me, mask), mine), device_id_type=MESH
        )
    pl.semaphore_wait(barrier, members - 1)
    copies = [
        pltpu.make_async_remote_copy(
            src_ref=count_ref,
            dst_ref=table_ref.at[me],
            send_sem=send_sem.at[mask],
            recv_sem=recv_sem.at[mask],
            device_id=(flip(me, mask), mine),
            device_id_type=MESH,
        )
        for mask in range(1, members)
    ]
    for copy in copies:
        copy.start()
    own_count = count_ref[...]
    table_ref[me] = own_count
    for copy in copies:
        copy.wait()
    row = lax.broadcasted_iota(jnp.int32, own_count.shape, 0)
    lane = lax.broadcasted_iota(jnp.int32, own_count.shape, 1)
    shift = members.bit_length() - 1
    start = jnp.zeros_like(own_count)
    first = jnp.zeros_like(own_count)
    slots = jnp.zeros_like(own_count)
    wanted = me + lane * members
    for member in range(members):
        count = table_ref[member]
        first = jnp.where(me == member, start, first)
        within = wanted - start
        holds = (within >= 0) & (within < count)
        slots = jnp.where(
            holds, member * per_owner + lax.shift_right_logical(within, shift), slots
        )
        start = start + count
    owner = jnp.zeros_like(lane)
    for member in range(1, members):
        owner = owner + (lane >= member * per_owner).astype(jnp.int32)
    layer = lane - owner * per_owner
    turned = (owner - first + members * NB) & (members - 1)
    chosen = jnp.minimum(turned + layer * members, NB - 1)
    chosen = jnp.maximum(chosen, 0)
    plan_ref[...] = jnp.where(row == 0, chosen, slots)


def make_plan(live_counts, members, per_owner):
    count = jnp.broadcast_to(live_counts[:, None], (8, 128))
    dma = pltpu.SemaphoreType.DMA
    return pl.pallas_call(
        functools.partial(plan_kernel, members, per_owner),
        out_shape=jax.ShapeDtypeStruct(count.shape, jnp.int32),
        in_specs=[pl.BlockSpec(memory_space=pltpu.VMEM)],
        out_specs=pl.BlockSpec(memory_space=pltpu.VMEM),
        scratch_shapes=[
            pltpu.VMEM((members,) + count.shape, jnp.int32), dma((members,)), dma((members,))
        ],
        compiler_params=pltpu.CompilerParams(collective_id=1, has_side_effects=True),
    )(count)


def exchange_kernel(
    members, columns, per_owner,
    sent_ref, weight_ref, far_weight_ref, held_ref, full_ref,
    local_sem, send_dp, recv_dp, send_x, recv_x, send_w, recv_w,
):
    me = lax.axis_index("dp")
    mine = lax.axis_index("mp")
    top = members // 2

    def dp_device(mask):
        return (flip(me, mask), mine)

    def mp_device(mask):
        return (me, flip(mine, mask))

    bits = [1 << b for b in reversed(range(columns.bit_length() - 1))]
    barrier = pltpu.get_barrier_semaphore()
    for mask in range(1, members):
        pl.semaphore_signal(barrier, inc=1, device_id=dp_device(mask), device_id_type=MESH)
    for mask in bits:
        pl.semaphore_signal(barrier, inc=1, device_id=mp_device(mask), device_id_type=MESH)
    pl.semaphore_wait(barrier, members - 1 + len(bits))

    def dp_copy(mask, layer, source):
        return pltpu.make_async_remote_copy(
            src_ref=sent_ref.at[flip(me, mask), layer],
            dst_ref=held_ref.at[mine, source, layer],
            send_sem=send_dp.at[mask, layer],
            recv_sem=recv_dp.at[mask, layer],
            device_id=dp_device(mask),
            device_id_type=MESH,
        )

    def mp_copy(place, bit, mask, layer):
        source = flip(me, mask)
        column = flip(mine, place)
        if mask == 0 and place == 0:
            src = sent_ref.at[source, layer]
        else:
            src = held_ref.at[column, source, layer]
        return pltpu.make_async_remote_copy(
            src_ref=src,
            dst_ref=held_ref.at[column, source, layer],
            send_sem=send_x.at[place ^ bit, mask, layer],
            recv_sem=recv_x.at[place ^ bit, mask, layer],
            device_id=mp_device(bit),
            device_id_type=MESH,
        )

    def weight_copy(mask, bit):
        owner = flip(me, mask)
        if mask == 0:
            src = weight_ref
        elif mask == top:
            src = far_weight_ref
        else:
            src = full_ref.at[owner]
        return pltpu.make_async_remote_copy(
            src_ref=src,
            dst_ref=full_ref.at[owner],
            send_sem=send_w.at[mask ^ bit],
            recv_sem=recv_w.at[mask ^ bit],
            device_id=dp_device(bit),
            device_id_type=MESH,
        )

    local = [
        pltpu.make_async_copy(weight_ref, full_ref.at[me], local_sem.at[0]),
        pltpu.make_async_copy(far_weight_ref, full_ref.at[flip(me, top)], local_sem.at[1]),
        pltpu.make_async_copy(sent_ref.at[me], held_ref.at[mine, me], local_sem.at[2]),
    ]
    started = []

    def start(copy):
        copy.start()
        started.append(copy)

    def spread_weight(mask, below):
        bit = below // 2
        while bit >= 1:
            start(weight_copy(mask, bit))
            bit //= 2

    def spread(place, below, mask, layer):
        for bit in bits:
            if bit < below:
                start(mp_copy(place, bit, mask, layer))

    order = sorted(range(1, members), key=lambda t: (-(bin(t).count("1") % 2), t))
    for layer in range(per_owner):
        spread(0, columns, 0, layer)
        for mask in order:
            start(dp_copy(mask, layer, me))
        if layer == 0:
            spread_weight(0, top)
            spread_weight(top, top)
    for copy in local:
        copy.start()

    chunks = [(0, layer) for layer in range(per_owner)]
    chunks += [(mask, layer) for layer in range(per_owner) for mask in order]
    weights = [t for t in range(1, members) if t != top]
    weights.sort(key=lambda t: (-(t & -t), t))
    lag = 3

    def relay(mask, layer):
        for place in range(1, columns):
            lowest = place & -place
            mp_copy(place ^ lowest, lowest, mask, layer).wait_recv()
            spread(place, lowest, mask, layer)

    for at in range(len(chunks) + lag):
        if at < len(chunks):
            mask, layer = chunks[at]
            if mask:
                dp_copy(mask, layer, me).wait_recv()
                spread(0, columns, mask, layer)
        if at >= members and at % 2 and weights:
            arrived = weights.pop(0)
            lowest = arrived & -arrived
            weight_copy(arrived ^ lowest, lowest).wait_recv()
            spread_weight(arrived, lowest)
        if at >= lag:
            relay(*chunks[at - lag])
    for arrived in weights:
        lowest = arrived & -arrived
        weight_copy(arrived ^ lowest, lowest).wait_recv()
        spread_weight(arrived, lowest)
    for copy in started:
        copy.wait_send()
    for copy in local:
        copy.wait()


def exchange(sent, weight, far_weight, members, columns):
    per_owner = sent.shape[1]
    anywhere = pl.BlockSpec(memory_space=pl.ANY)
    dma = pltpu.SemaphoreType.DMA
    return pl.pallas_call(
        functools.partial(exchange_kernel, members, columns, per_owner),
        out_shape=(
            jax.ShapeDtypeStruct((columns,) + sent.shape, sent.dtype),
            jax.ShapeDtypeStruct((members,) + weight.shape, weight.dtype),
        ),
        in_specs=[anywhere] * 3,
        out_specs=(anywhere, anywhere),
        scratch_shapes=[
            dma((3,)),
            dma((members, per_owner)),
            dma((members, per_owner)),
            dma((columns, members, per_owner)),
            dma((columns, members, per_owner)),
            dma((members,)),
            dma((members,)),
        ],
        compiler_params=pltpu.CompilerParams(collective_id=0, has_side_effects=True, vmem_limit_bytes=VMEM),
        cost_estimate=pl.CostEstimate(
            flops=0, bytes_accessed=60 * sent.size, transcendentals=0
        ),
    )(sent, weight, far_weight)


def project_kernel(columns, slots_ref, first_ref, second_ref, weight_ref, out_ref):
    total = None
    for column in range(columns):
        rows = jnp.concatenate([first_ref[column, 0], second_ref[column, 0]], axis=0)
        depth = rows.shape[1]
        part = jnp.dot(
            rows, weight_ref[column * depth:(column + 1) * depth, :],
            preferred_element_type=jnp.float32,
        )
        total = part if total is None else total + part
    out_ref[...] = total.astype(out_ref.dtype)


def project(slots, held, weight, kept):
    columns, total, _, depth = held.shape
    width = weight.shape[1]

    def picked(which):
        return pl.BlockSpec(
            (columns, 1, BLOCK, depth), lambda i, s: (0, s[1, 2 * i + which], 0, 0)
        )

    return pl.pallas_call(
        functools.partial(project_kernel, columns),
        out_shape=jax.ShapeDtypeStruct((kept * BLOCK, width), jnp.bfloat16),
        grid_spec=pltpu.PrefetchScalarGridSpec(
            num_scalar_prefetch=1,
            grid=(kept // 2,),
            in_specs=[
                picked(0),
                picked(1),
                pl.BlockSpec(weight.shape, lambda i, s: (0, 0)),
            ],
            out_specs=pl.BlockSpec((2 * BLOCK, width), lambda i, s: (i, 0)),
        ),
        compiler_params=pltpu.CompilerParams(vmem_limit_bytes=VMEM),
    )(slots, held, held, weight)


PIECES = 4
LAG = 4


def attend_block(block, queries_ref, keys_ref, values_ref, ids_ref, out_ref, owner, layer):
    repeat = queries_ref.shape[2] // HEAD_SIZE
    factor = math.log2(math.e) / math.sqrt(HEAD_SIZE)
    row_at = lax.broadcasted_iota(jnp.int32, (BLOCK, BLOCK), 0)
    col_at = lax.broadcasted_iota(jnp.int32, (BLOCK, BLOCK), 1)
    ones = jnp.ones((BLOCK, HEAD_SIZE), jnp.bfloat16)
    along = jnp.broadcast_to(ids_ref[block], (BLOCK, BLOCK))
    down = along.T
    bias = jnp.where((along == down) & (col_at <= row_at), 0.0, MASKED)
    value = jnp.where(down >= 0, values_ref[block].astype(jnp.float32), 0.0)
    value = jnp.concatenate([value.astype(jnp.bfloat16), ones], axis=1)
    key = keys_ref[block]
    query = queries_ref[block]
    query = jnp.concatenate(
        [query[:, h * HEAD_SIZE:(h + 1) * HEAD_SIZE] for h in range(repeat)], axis=0
    )
    scores = lax.dot_general(
        query, key, (((1,), (1,)), ((), ())), preferred_element_type=jnp.float32
    )
    weights = []
    for head in range(repeat):
        part = scores[head * BLOCK:(head + 1) * BLOCK] + bias
        highest = jnp.max(part, axis=1, keepdims=True)
        weights.append(jnp.exp2((part - highest) * factor).astype(jnp.bfloat16))
    summed = jnp.dot(
        jnp.concatenate(weights, axis=0), value, preferred_element_type=jnp.float32
    )
    summed = summed[:, :HEAD_SIZE] / summed[:, HEAD_SIZE:]
    for head in range(repeat):
        columns = slice(head * HEAD_SIZE, (head + 1) * HEAD_SIZE)
        out_ref[owner, layer * BLOCK:(layer + 1) * BLOCK, columns] = summed[
            head * BLOCK:(head + 1) * BLOCK
        ].astype(out_ref.dtype)


def differ(one, two, members):
    total, bit = 0, 1
    while bit < members:
        total = total + bit * ((one // bit + two // bit) % 2)
        bit *= 2
    return total


def merge(first, second, one=1, two=1):
    first, second, out = list(first), list(second), []
    while first or second:
        for _ in range(one):
            if first:
                out += first.pop(0)
        for _ in range(two):
            if second:
                out += second.pop(0)
    return out


def after_sends(near_middle, layers):
    pieces = range(PIECES)
    block = range(layers)
    far = [(m, l) for l in block for m in (7, 5, 6, 4)]
    near = [("a", m, l) for l in block for m in (2, 3)]
    out = []
    if near_middle:
        early = [("a", m, l) for m, l in far if m in (4, 5)]
        late = [("a", m, l) for m, l in far if m in (6, 7)]
        out += [("w", 6, p) for p in pieces]
        out += [("a", 1, l) for l in block]
        out += merge([[("w", 4, p)] for p in pieces], [[n] for n in near[:3]])
        out += near[3:]
        out += [("need", 1), ("need", 3), ("P", 0)]
        out += early[:3] + [("P", 2)] + early[3:]
        out += late[:4] + [("P", 4), ("need", 7), ("need", 5), ("Q", 0), ("Q", 2)]
        out += late[4:5] + [("Q", 4)] + late[5:]
    else:
        early = [("a", m, l) for m, l in far if m in (6, 7)]
        late = [("a", m, l) for m, l in far if m in (4, 5)]
        out += [("a", 1, l) for l in block]
        out += near
        out += [("need", 1), ("need", 3), ("P", 0)]
        out += merge([[("w", 4, p)] for p in pieces], [[e] for e in early[:3]])
        out += [("P", 2)]
        out += merge([[("w", 6, p)] for p in pieces], [[e] for e in early[3:]])
        out += late[:4] + [("P", 4)] + late[4:5]
        out += [("need", 5), ("need", 7), ("Q", 0), ("Q", 2), ("Q", 4)] + late[5:]
    out += [("F", l) for l in block]
    return with_relays(out, near_middle, layers)


def with_relays(ops, near_middle, layers):
    turn = 1 if near_middle else 3
    units = [0, 1, 2, 3] + [u ^ turn for u in (4, 5, 6, 7)]
    waiting = [(0, l) for l in range(layers)]
    arrived, out = [], []

    def settle(wanted):
        while any(w in waiting for w in wanted):
            out.append(("x",) + waiting[0])
            arrived.append(waiting.pop(0))
        for w in wanted:
            if w in arrived:
                out.append(("c",) + w)
                arrived.remove(w)

    for op in ops:
        if op[0] == "P":
            settle([(units[u], l) for u in (op[1], op[1] + 1) for l in range(layers)])
        elif op[0] == "F":
            settle([(units[u], op[1]) for u in (6, 7)])
        out.append(op)
        if op[0] == "a":
            waiting.append(op[1:])
            if len(waiting) > LAG:
                out.append(("x",) + waiting[0])
                arrived.append(waiting.pop(0))
    return out


def fused_kernel(
    members, columns, layers,
    queries_hbm, keys_hbm, values_hbm, ids_hbm, count_ref, weight_hbm,
    plan_ref, out_hbm,
    queries_ref, keys_ref, values_ref, ids_ref, table_ref, own_ref, spot_ref,
    sent_ref, held_ref, full_ref, acc_ref, done_ref,
    in_sem, spot_sem, out_sem, send_n, recv_n, send_a, recv_a,
    send_x, recv_x, send_c, recv_c, send_w, recv_w,
):
    me = lax.axis_index("dp")
    mine = lax.axis_index("mp")
    ring = me // 2
    middle = ((ring + 1) // 2) % 2
    inner = middle == 1
    outer = middle == 0
    half = ring // 2
    owned = weight_hbm.shape[0]
    piece = owned // PIECES
    depth = sent_ref.shape[2]
    reach = columns // 2 * depth

    inputs = [
        pltpu.make_async_copy(ids_hbm, ids_ref, in_sem.at[0]),
        pltpu.make_async_copy(keys_hbm, keys_ref, in_sem.at[1]),
        pltpu.make_async_copy(values_hbm, values_ref, in_sem.at[2]),
        pltpu.make_async_copy(queries_hbm, queries_ref, in_sem.at[3]),
        pltpu.make_async_copy(
            weight_hbm,
            full_ref.at[pl.ds(pl.multiple_of(me * owned, owned), owned)],
            in_sem.at[4],
        ),
    ]
    for copy in inputs:
        copy.start()
    own_ref[...] = jnp.full(own_ref.shape, count_ref[0], jnp.int32)

    barrier = pltpu.get_barrier_semaphore()
    for mask in range(1, members):
        pl.semaphore_signal(
            barrier, inc=1, device_id=(flip(me, mask), mine), device_id_type=MESH
        )
    for mask in (1, 2):
        pl.semaphore_signal(
            barrier, inc=1, device_id=(me, flip(mine, mask)), device_id_type=MESH
        )
    pl.semaphore_wait(barrier, members + 1)

    def remote(src, dst, send, recv, device):
        return pltpu.make_async_remote_copy(
            src_ref=src, dst_ref=dst, send_sem=send, recv_sem=recv,
            device_id=device, device_id_type=MESH,
        )

    def count_copy(mask):
        return remote(
            own_ref, table_ref.at[me], send_n.at[mask], recv_n.at[mask], (flip(me, mask), mine)
        )

    def rows_of(layer):
        return pl.ds(layer * BLOCK, BLOCK)

    def block_copy(mask, layer):
        return remote(
            sent_ref.at[flip(me, mask), rows_of(layer)],
            held_ref.at[mine, me, rows_of(layer)],
            send_a.at[mask, layer], recv_a.at[mask, layer],
            (flip(me, mask), mine),
        )

    def x_copy(mask, layer):
        source = flip(me, mask)
        src = held_ref.at[mine, source, rows_of(layer)]
        if mask == 0:
            src = sent_ref.at[me, rows_of(layer)]
        return remote(
            src, held_ref.at[mine, source, rows_of(layer)],
            send_x.at[mask, layer], recv_x.at[mask, layer],
            (me, flip(mine, 2)),
        )

    def core_copy(mask, layer, far):
        source = flip(me, mask)
        column = flip(mine, 2 * far)
        src = held_ref.at[column, source, rows_of(layer)]
        if mask == 0 and not far:
            src = sent_ref.at[me, rows_of(layer)]
        return remote(
            src, held_ref.at[column, source, rows_of(layer)],
            send_c.at[far, mask, layer], recv_c.at[far, mask, layer],
            (me, flip(mine, 1)),
        )

    def weight_copy(mask, to, part):
        first = pl.multiple_of(flip(me, mask) * owned + part * piece, piece)
        src = full_ref.at[pl.ds(first, piece)]
        if mask == 0:
            src = weight_hbm.at[pl.ds(pl.multiple_of(part * piece, piece), piece)]
        return remote(
            src, full_ref.at[pl.ds(first, piece)],
            send_w.at[mask // 2, to // 2, part], recv_w.at[mask ^ to, part],
            (flip(me, to), mine),
        )

    always, at_inner, at_outer = [], [], []

    def start(kept, make, *where):
        make(*where).start()
        kept.append((make, where))

    for mask in range(1, members):
        start(always, count_copy, mask)

    @pl.when(inner)
    def _():
        for part in range(PIECES):
            start(at_inner, weight_copy, 0, 6, part)

    for part in range(PIECES):
        start(always, weight_copy, 0, 2, part)
    for part in range(PIECES // 2):
        start(always, weight_copy, 0, 1, part)

    table_ref[me] = own_ref[...]
    for mask in range(1, members):
        count_copy(mask).wait_recv()
    lane = lax.broadcasted_iota(jnp.int32, own_ref.shape, 1)
    shift = members.bit_length() - 1
    begin = jnp.zeros(own_ref.shape, jnp.int32)
    first = jnp.zeros(own_ref.shape, jnp.int32)
    slots = jnp.zeros(own_ref.shape, jnp.int32)
    wanted = me + lane * members
    for member in range(members):
        count = table_ref[member]
        first = jnp.where(me == member, begin, first)
        within = wanted - begin
        holds = (within >= 0) & (within < count)
        slots = jnp.where(
            holds, member * layers + lax.shift_right_logical(within, shift), slots
        )
        begin = begin + count
    plan_ref[...] = slots
    table_ref[me] = first
    spot = pltpu.make_async_copy(table_ref.at[me], spot_ref, spot_sem)
    spot.start()
    for copy in inputs[:4]:
        copy.wait()
    spot.wait()
    turn = members * NB - spot_ref[0, 0]

    def attend_for(at):
        owner = differ(me, flip(at, 1), members)
        block = (owner + turn) & (members - 1)
        for layer in range(layers):
            attend_block(
                block + layer * members,
                queries_ref, keys_ref, values_ref, ids_ref, sent_ref, owner, layer,
            )

    @pl.loop(0, 2)
    def _(at):
        attend_for(at)

    for layer in range(layers):
        start(always, block_copy, 1, layer)
        start(always, x_copy, 0, layer)
        start(always, core_copy, 0, layer, 0)
    for part in range(PIECES // 2, PIECES):
        start(always, weight_copy, 0, 1, part)
    held_ref[mine, me] = sent_ref[me]

    @pl.loop(2, 4)
    def _(at):
        attend_for(at)

    for layer in range(layers):
        for mask in (2, 3):
            start(always, block_copy, mask, layer)

    @pl.loop(4, 8)
    def _(at):
        attend_for(at)
        weight_copy(0, 2, at - 4).wait_recv()
        weight_copy(2, 1, at - 4).start()

        @pl.when(inner)
        def _():
            weight_copy(2, 6, at - 4).start()

    always.extend((weight_copy, (2, 1, part)) for part in range(PIECES))
    at_inner.extend((weight_copy, (2, 6, part)) for part in range(PIECES))
    for layer in range(layers):
        for mask in (7, 5, 6, 4):
            start(always, block_copy, mask, layer)
    inputs[4].wait()

    tile = 256
    width = full_ref.shape[1]

    def source_of(at):
        early = (at // 4 + 1) % 2
        far = flip(at, 1) * middle + flip(at, 3) * (1 - middle)
        return differ(me, early * at + (1 - early) * far, members)

    def part_of(which, source, rows, lanes):
        total = None
        for column in range(columns // 2):
            row = pl.multiple_of(which * reach + column * depth, depth)
            part = jnp.dot(
                held_ref[which * (columns // 2) + column, source, rows, :],
                full_ref[pl.ds(row, depth), lanes],
                preferred_element_type=jnp.float32,
            )
            total = part if total is None else total + part
        return total

    every = pl.ds(0, layers * BLOCK)

    def near_product(at):
        source = source_of(at)
        for lane_at in range(0, width, tile):
            lanes = pl.ds(lane_at, tile)
            acc_ref[at, :, lanes] = part_of(half, source, every, lanes)

    def write(at, rows, sem):
        source = source_of(at)
        return pltpu.make_async_copy(
            done_ref.at[at, rows], out_hbm.at[source, rows], sem
        )

    def far_product(at):
        source = source_of(at)
        for lane_at in range(0, width, tile):
            lanes = pl.ds(lane_at, tile)
            total = acc_ref[at, :, lanes] + part_of(1 - half, source, every, lanes)
            done_ref[at, :, lanes] = total.astype(done_ref.dtype)
        write(at, every, out_sem.at[at, 0]).start()

    def whole_product(at, layer):
        source = source_of(at)
        rows = rows_of(layer)
        for lane_at in range(0, width, tile):
            lanes = pl.ds(lane_at, tile)
            total = part_of(half, source, rows, lanes)
            total = total + part_of(1 - half, source, rows, lanes)
            done_ref[at, rows, lanes] = total.astype(done_ref.dtype)
        write(at, rows, out_sem.at[at, layer]).start()

    def product(kind, which):
        if kind == "P":
            pl.loop(which, which + 2)(near_product)
        elif kind == "Q":
            pl.loop(which, which + 2)(far_product)
        else:
            pl.loop(6, 8)(lambda at: whole_product(at, which))

    def step(op, near_middle, kept):
        kind = op[0]
        if kind == "a":
            block_copy(*op[1:]).wait_recv()
            start(kept, x_copy, *op[1:])
            start(kept, core_copy, *op[1:], 0)
        elif kind == "x":
            x_copy(*op[1:]).wait_recv()
            start(kept, core_copy, *op[1:], 1)
        elif kind == "c":
            core_copy(*op[1:], 0).wait_recv()
            core_copy(*op[1:], 1).wait_recv()
        elif kind == "need":
            for part in range(PIECES):
                weight_copy(0, op[1], part).wait_recv()
        elif kind == "w":
            mask, part = op[1:]
            weight_copy(0, mask, part).wait_recv()
            if near_middle:
                start(kept, weight_copy, mask, 2, part)
            start(kept, weight_copy, mask, 1, part)

    plans = [after_sends(True, layers), after_sends(False, layers)]
    while plans[0]:
        stop = None
        for plan, near_middle, kept, here in (
            (plans[0], True, at_inner, inner), (plans[1], False, at_outer, outer)
        ):
            ops = []
            while plan and plan[0][0] not in ("P", "Q", "F"):
                ops.append(plan.pop(0))
            if ops:

                @pl.when(here)
                def _(ops=ops, near_middle=near_middle, kept=kept):
                    for op in ops:
                        step(op, near_middle, kept)

            if plan:
                stop = plan.pop(0)
        if stop is not None:
            product(*stop)

    for kept, here in ((at_inner, inner), (at_outer, outer)):

        @pl.when(here)
        def _(kept=kept):
            for make, where in kept:
                make(*where).wait_send()

    for make, where in always:
        make(*where).wait_send()
    for at in range(members):
        if at < 6:
            write(at, every, out_sem.at[at, 0]).wait()
        else:
            for layer in range(layers):
                write(at, rows_of(layer), out_sem.at[at, layer]).wait()


def fused(queries, keys, values, ids, live_counts, weight, members, columns, layers):
    anywhere = pl.BlockSpec(memory_space=pl.ANY)
    dma = pltpu.SemaphoreType.DMA
    rows = layers * BLOCK
    depth = queries.shape[2]
    width = weight.shape[1]
    low = jnp.bfloat16
    return pl.pallas_call(
        functools.partial(fused_kernel, members, columns, layers),
        out_shape=(
            jax.ShapeDtypeStruct((8, 128), jnp.int32),
            jax.ShapeDtypeStruct((members, rows, width), low),
        ),
        in_specs=[anywhere] * 4 + [pl.BlockSpec(memory_space=pltpu.SMEM), anywhere],
        out_specs=(pl.BlockSpec(memory_space=pltpu.VMEM), anywhere),
        scratch_shapes=[
            pltpu.VMEM(queries.shape, low),
            pltpu.VMEM(keys.shape, low),
            pltpu.VMEM(values.shape, low),
            pltpu.VMEM(ids.shape, jnp.int32),
            pltpu.VMEM((members, 8, 128), jnp.int32),
            pltpu.VMEM((8, 128), jnp.int32),
            pltpu.SMEM((8, 128), jnp.int32),
            pltpu.VMEM((members, rows, depth), low),
            pltpu.VMEM((columns, members, rows, depth), low),
            pltpu.VMEM((members * weight.shape[0], width), low),
            pltpu.VMEM((6, rows, width), jnp.float32),
            pltpu.VMEM((members, rows, width), low),
            dma((5,)),
            dma,
            dma((members, layers)),
            dma((members,)), dma((members,)),
            dma((members, layers)), dma((members, layers)),
            dma((members, layers)), dma((members, layers)),
            dma((2, members, layers)), dma((2, members, layers)),
            dma((4, 4, PIECES)), dma((members, PIECES)),
        ],
        compiler_params=pltpu.CompilerParams(
            collective_id=2, has_side_effects=True, vmem_limit_bytes=VMEM
        ),
    )(queries, keys, values, ids, live_counts, weight)


def order_kernel(slots_ref, first_ref, second_ref, out_ref):
    out_ref[:BLOCK] = first_ref[0]
    out_ref[BLOCK:] = second_ref[0]


def in_order(slots, products, kept):
    width = products.shape[2]

    def picked(which):
        return pl.BlockSpec((1, BLOCK, width), lambda i, s: (s[0, 2 * i + which], 0, 0))

    return pl.pallas_call(
        order_kernel,
        out_shape=jax.ShapeDtypeStruct((kept * BLOCK, width), products.dtype),
        grid_spec=pltpu.PrefetchScalarGridSpec(
            num_scalar_prefetch=1,
            grid=(kept // 2,),
            in_specs=[picked(0), picked(1)],
            out_specs=pl.BlockSpec((2 * BLOCK, width), lambda i, s: (i, 0)),
        ),
        compiler_params=pltpu.CompilerParams(vmem_limit_bytes=VMEM),
    )(slots, products, products)


def body(members, columns, queries, keys, values, doc_ids, live_counts, out_weight):
    per_owner = (NB + members - 1) // members
    kept = NB * 11 // 12
    half = members // 2
    if members == 8 and columns == 4:
        slots, products = fused(
            queries.reshape(NB, BLOCK, -1), keys.reshape(NB, BLOCK, -1),
            values.reshape(NB, BLOCK, -1), doc_ids.reshape(NB, 1, BLOCK),
            live_counts, out_weight,
            members, columns, per_owner,
        )
        products = products.reshape(members * per_owner, BLOCK, out_weight.shape[1])
        return in_order(slots, products, kept)
    plan = make_plan(live_counts, members, per_owner)
    plan, near_weight = lax.optimization_barrier((plan, out_weight))
    far_weight = lax.ppermute(
        near_weight, "dp", [(i, (i + half) % members) for i in range(members)]
    )
    sent = attend(
        plan, queries, keys, values, doc_ids.reshape(NB, BLOCK), members, per_owner
    )
    held, full = exchange(sent, out_weight, far_weight, members, columns)
    held = held.reshape(columns, members * per_owner, BLOCK, queries.shape[1])
    full = full.reshape(members * out_weight.shape[0], out_weight.shape[1])
    return project(plan, held, full, kept)


def solution(mesh):
    return jax.shard_map(
        functools.partial(body, mesh.shape["dp"], mesh.shape["mp"]),
        mesh=mesh,
        in_specs=(P("dp", "mp"), P("dp", "mp"), P("dp", "mp"), P("dp"), P("dp"), P("dp", "mp")),
        out_specs=P("dp", "mp"),
        check_vma=False,
    )
```

```python
import functools
import math

import jax
import jax.numpy as jnp
from jax import lax
from jax.experimental import pallas as pl
from jax.experimental.pallas import tpu as pltpu
from jax.sharding import PartitionSpec as P

HEAD_SIZE = 128
BLOCK = 128
NB = 24
MESH = pl.DeviceIdType.MESH
MASKED = -1e30
VMEM = 60 * 1024 * 1024


def attend_kernel(per_owner, plan_ref, queries_ref, keys_ref, values_ref, ids_ref, out_ref):
    step = pl.program_id(0)
    repeat = queries_ref.shape[1] // HEAD_SIZE
    factor = math.log2(math.e) / math.sqrt(HEAD_SIZE)
    row_at = lax.broadcasted_iota(jnp.int32, (BLOCK, BLOCK), 0)
    col_at = lax.broadcasted_iota(jnp.int32, (BLOCK, BLOCK), 1)
    causal = col_at <= row_at
    ones = jnp.ones((BLOCK, HEAD_SIZE), jnp.bfloat16)
    for layer in range(per_owner):
        block = plan_ref[0, step * per_owner + layer]
        rows = pl.ds(pl.multiple_of(block * BLOCK, BLOCK), BLOCK)
        along = jnp.broadcast_to(ids_ref[pl.ds(block, 1), :], (BLOCK, BLOCK))
        down = along.T
        bias = jnp.where((along == down) & causal, 0.0, MASKED)
        value = jnp.where(down >= 0, values_ref[rows, :].astype(jnp.float32), 0.0)
        value = jnp.concatenate([value.astype(jnp.bfloat16), ones], axis=1)
        key = keys_ref[rows, :]
        query = queries_ref[rows, :]
        query = jnp.concatenate(
            [query[:, h * HEAD_SIZE:(h + 1) * HEAD_SIZE] for h in range(repeat)], axis=0
        )
        scores = lax.dot_general(
            query, key, (((1,), (1,)), ((), ())), preferred_element_type=jnp.float32
        )
        weights = []
        for head in range(repeat):
            part = scores[head * BLOCK:(head + 1) * BLOCK] + bias
            highest = jnp.max(part, axis=1, keepdims=True)
            weights.append(jnp.exp2((part - highest) * factor).astype(jnp.bfloat16))
        summed = jnp.dot(
            jnp.concatenate(weights, axis=0), value, preferred_element_type=jnp.float32
        )
        summed = summed[:, :HEAD_SIZE] / summed[:, HEAD_SIZE:]
        for head in range(repeat):
            columns = slice(head * HEAD_SIZE, (head + 1) * HEAD_SIZE)
            out_ref[0, layer, :, columns] = summed[head * BLOCK:(head + 1) * BLOCK].astype(
                out_ref.dtype
            )


def attend(plan, queries, keys, values, ids, members, per_owner):
    cols = queries.shape[1]

    def whole(array):
        return pl.BlockSpec(array.shape, lambda i, c: (0, 0))

    return pl.pallas_call(
        functools.partial(attend_kernel, per_owner),
        out_shape=jax.ShapeDtypeStruct((members, per_owner, BLOCK, cols), jnp.bfloat16),
        grid_spec=pltpu.PrefetchScalarGridSpec(
            num_scalar_prefetch=1,
            grid=(members,),
            in_specs=[whole(queries), whole(keys), whole(values), whole(ids)],
            out_specs=pl.BlockSpec((1, per_owner, BLOCK, cols), lambda i, c: (i, 0, 0, 0)),
        ),
        compiler_params=pltpu.CompilerParams(vmem_limit_bytes=VMEM),
        cost_estimate=pl.CostEstimate(
            flops=members * per_owner * cols * BLOCK * BLOCK * 4,
            bytes_accessed=4 * queries.size,
            transcendentals=members * per_owner * cols * BLOCK,
        ),
    )(plan, queries, keys, values, ids)


def flip(index, mask):
    bit = 1
    while bit <= mask:
        if mask & bit:
            index = index + bit - 2 * bit * ((index // bit) % 2)
        bit *= 2
    return index


def plan_kernel(members, per_owner, count_ref, plan_ref, table_ref, send_sem, recv_sem):
    me = lax.axis_index("dp")
    mine = lax.axis_index("mp")
    barrier = pltpu.get_barrier_semaphore()
    for mask in range(1, members):
        pl.semaphore_signal(
            barrier, inc=1, device_id=(flip(me, mask), mine), device_id_type=MESH
        )
    pl.semaphore_wait(barrier, members - 1)
    copies = [
        pltpu.make_async_remote_copy(
            src_ref=count_ref,
            dst_ref=table_ref.at[me],
            send_sem=send_sem.at[mask],
            recv_sem=recv_sem.at[mask],
            device_id=(flip(me, mask), mine),
            device_id_type=MESH,
        )
        for mask in range(1, members)
    ]
    for copy in copies:
        copy.start()
    own_count = count_ref[...]
    table_ref[me] = own_count
    for copy in copies:
        copy.wait()
    row = lax.broadcasted_iota(jnp.int32, own_count.shape, 0)
    lane = lax.broadcasted_iota(jnp.int32, own_count.shape, 1)
    shift = members.bit_length() - 1
    start = jnp.zeros_like(own_count)
    first = jnp.zeros_like(own_count)
    slots = jnp.zeros_like(own_count)
    wanted = me + lane * members
    for member in range(members):
        count = table_ref[member]
        first = jnp.where(me == member, start, first)
        within = wanted - start
        holds = (within >= 0) & (within < count)
        slots = jnp.where(
            holds, member * per_owner + lax.shift_right_logical(within, shift), slots
        )
        start = start + count
    owner = jnp.zeros_like(lane)
    for member in range(1, members):
        owner = owner + (lane >= member * per_owner).astype(jnp.int32)
    layer = lane - owner * per_owner
    turned = (owner - first + members * NB) & (members - 1)
    chosen = jnp.minimum(turned + layer * members, NB - 1)
    chosen = jnp.maximum(chosen, 0)
    plan_ref[...] = jnp.where(row == 0, chosen, slots)


def make_plan(live_counts, members, per_owner):
    count = jnp.broadcast_to(live_counts[:, None], (8, 128))
    dma = pltpu.SemaphoreType.DMA
    return pl.pallas_call(
        functools.partial(plan_kernel, members, per_owner),
        out_shape=jax.ShapeDtypeStruct(count.shape, jnp.int32),
        in_specs=[pl.BlockSpec(memory_space=pltpu.VMEM)],
        out_specs=pl.BlockSpec(memory_space=pltpu.VMEM),
        scratch_shapes=[
            pltpu.VMEM((members,) + count.shape, jnp.int32), dma((members,)), dma((members,))
        ],
        compiler_params=pltpu.CompilerParams(collective_id=1, has_side_effects=True),
    )(count)


def exchange_kernel(
    members, columns, per_owner,
    sent_ref, weight_ref, far_weight_ref, held_ref, full_ref,
    local_sem, send_dp, recv_dp, send_x, recv_x, send_w, recv_w,
):
    me = lax.axis_index("dp")
    mine = lax.axis_index("mp")
    top = members // 2

    def dp_device(mask):
        return (flip(me, mask), mine)

    def mp_device(mask):
        return (me, flip(mine, mask))

    bits = [1 << b for b in reversed(range(columns.bit_length() - 1))]
    barrier = pltpu.get_barrier_semaphore()
    for mask in range(1, members):
        pl.semaphore_signal(barrier, inc=1, device_id=dp_device(mask), device_id_type=MESH)
    for mask in bits:
        pl.semaphore_signal(barrier, inc=1, device_id=mp_device(mask), device_id_type=MESH)
    pl.semaphore_wait(barrier, members - 1 + len(bits))

    def dp_copy(mask, layer, source):
        return pltpu.make_async_remote_copy(
            src_ref=sent_ref.at[flip(me, mask), layer],
            dst_ref=held_ref.at[mine, source, layer],
            send_sem=send_dp.at[mask, layer],
            recv_sem=recv_dp.at[mask, layer],
            device_id=dp_device(mask),
            device_id_type=MESH,
        )

    def mp_copy(place, bit, mask, layer):
        source = flip(me, mask)
        column = flip(mine, place)
        if mask == 0 and place == 0:
            src = sent_ref.at[source, layer]
        else:
            src = held_ref.at[column, source, layer]
        return pltpu.make_async_remote_copy(
            src_ref=src,
            dst_ref=held_ref.at[column, source, layer],
            send_sem=send_x.at[place ^ bit, mask, layer],
            recv_sem=recv_x.at[place ^ bit, mask, layer],
            device_id=mp_device(bit),
            device_id_type=MESH,
        )

    def weight_copy(mask, bit):
        owner = flip(me, mask)
        if mask == 0:
            src = weight_ref
        elif mask == top:
            src = far_weight_ref
        else:
            src = full_ref.at[owner]
        return pltpu.make_async_remote_copy(
            src_ref=src,
            dst_ref=full_ref.at[owner],
            send_sem=send_w.at[mask ^ bit],
            recv_sem=recv_w.at[mask ^ bit],
            device_id=dp_device(bit),
            device_id_type=MESH,
        )

    local = [
        pltpu.make_async_copy(weight_ref, full_ref.at[me], local_sem.at[0]),
        pltpu.make_async_copy(far_weight_ref, full_ref.at[flip(me, top)], local_sem.at[1]),
        pltpu.make_async_copy(sent_ref.at[me], held_ref.at[mine, me], local_sem.at[2]),
    ]
    started = []

    def start(copy):
        copy.start()
        started.append(copy)

    def spread_weight(mask, below):
        bit = below // 2
        while bit >= 1:
            start(weight_copy(mask, bit))
            bit //= 2

    def spread(place, below, mask, layer):
        for bit in bits:
            if bit < below:
                start(mp_copy(place, bit, mask, layer))

    order = sorted(range(1, members), key=lambda t: (-(bin(t).count("1") % 2), t))
    for layer in range(per_owner):
        spread(0, columns, 0, layer)
        for mask in order:
            start(dp_copy(mask, layer, me))
        if layer == 0:
            spread_weight(0, top)
            spread_weight(top, top)
    for copy in local:
        copy.start()

    chunks = [(0, layer) for layer in range(per_owner)]
    chunks += [(mask, layer) for layer in range(per_owner) for mask in order]
    weights = [t for t in range(1, members) if t != top]
    weights.sort(key=lambda t: (-(t & -t), t))
    lag = 3

    def relay(mask, layer):
        for place in range(1, columns):
            lowest = place & -place
            mp_copy(place ^ lowest, lowest, mask, layer).wait_recv()
            spread(place, lowest, mask, layer)

    for at in range(len(chunks) + lag):
        if at < len(chunks):
            mask, layer = chunks[at]
            if mask:
                dp_copy(mask, layer, me).wait_recv()
                spread(0, columns, mask, layer)
        if at >= members and at % 2 and weights:
            arrived = weights.pop(0)
            lowest = arrived & -arrived
            weight_copy(arrived ^ lowest, lowest).wait_recv()
            spread_weight(arrived, lowest)
        if at >= lag:
            relay(*chunks[at - lag])
    for arrived in weights:
        lowest = arrived & -arrived
        weight_copy(arrived ^ lowest, lowest).wait_recv()
        spread_weight(arrived, lowest)
    for copy in started:
        copy.wait_send()
    for copy in local:
        copy.wait()


def exchange(sent, weight, far_weight, members, columns):
    per_owner = sent.shape[1]
    anywhere = pl.BlockSpec(memory_space=pl.ANY)
    dma = pltpu.SemaphoreType.DMA
    return pl.pallas_call(
        functools.partial(exchange_kernel, members, columns, per_owner),
        out_shape=(
            jax.ShapeDtypeStruct((columns,) + sent.shape, sent.dtype),
            jax.ShapeDtypeStruct((members,) + weight.shape, weight.dtype),
        ),
        in_specs=[anywhere] * 3,
        out_specs=(anywhere, anywhere),
        scratch_shapes=[
            dma((3,)),
            dma((members, per_owner)),
            dma((members, per_owner)),
            dma((columns, members, per_owner)),
            dma((columns, members, per_owner)),
            dma((members,)),
            dma((members,)),
        ],
        compiler_params=pltpu.CompilerParams(collective_id=0, has_side_effects=True, vmem_limit_bytes=VMEM),
        cost_estimate=pl.CostEstimate(
            flops=0, bytes_accessed=60 * sent.size, transcendentals=0
        ),
    )(sent, weight, far_weight)


def project_kernel(columns, slots_ref, first_ref, second_ref, weight_ref, out_ref):
    total = None
    for column in range(columns):
        rows = jnp.concatenate([first_ref[column, 0], second_ref[column, 0]], axis=0)
        depth = rows.shape[1]
        part = jnp.dot(
            rows, weight_ref[column * depth:(column + 1) * depth, :],
            preferred_element_type=jnp.float32,
        )
        total = part if total is None else total + part
    out_ref[...] = total.astype(out_ref.dtype)


def project(slots, held, weight, kept):
    columns, total, _, depth = held.shape
    width = weight.shape[1]

    def picked(which):
        return pl.BlockSpec(
            (columns, 1, BLOCK, depth), lambda i, s: (0, s[1, 2 * i + which], 0, 0)
        )

    return pl.pallas_call(
        functools.partial(project_kernel, columns),
        out_shape=jax.ShapeDtypeStruct((kept * BLOCK, width), jnp.bfloat16),
        grid_spec=pltpu.PrefetchScalarGridSpec(
            num_scalar_prefetch=1,
            grid=(kept // 2,),
            in_specs=[
                picked(0),
                picked(1),
                pl.BlockSpec(weight.shape, lambda i, s: (0, 0)),
            ],
            out_specs=pl.BlockSpec((2 * BLOCK, width), lambda i, s: (i, 0)),
        ),
        compiler_params=pltpu.CompilerParams(vmem_limit_bytes=VMEM),
    )(slots, held, held, weight)


PIECES = 4
LAG = 4


def attend_block(block, queries_ref, keys_ref, values_ref, ids_ref, out_ref, owner, layer):
    repeat = queries_ref.shape[2] // HEAD_SIZE
    factor = math.log2(math.e) / math.sqrt(HEAD_SIZE)
    row_at = lax.broadcasted_iota(jnp.int32, (BLOCK, BLOCK), 0)
    col_at = lax.broadcasted_iota(jnp.int32, (BLOCK, BLOCK), 1)
    ones = jnp.ones((BLOCK, HEAD_SIZE), jnp.bfloat16)
    along = jnp.broadcast_to(ids_ref[block], (BLOCK, BLOCK))
    down = along.T
    bias = jnp.where((along == down) & (col_at <= row_at), 0.0, MASKED)
    value = jnp.where(down >= 0, values_ref[block].astype(jnp.float32), 0.0)
    value = jnp.concatenate([value.astype(jnp.bfloat16), ones], axis=1)
    key = keys_ref[block]
    query = queries_ref[block]
    query = jnp.concatenate(
        [query[:, h * HEAD_SIZE:(h + 1) * HEAD_SIZE] for h in range(repeat)], axis=0
    )
    scores = lax.dot_general(
        query, key, (((1,), (1,)), ((), ())), preferred_element_type=jnp.float32
    )
    weights = []
    for head in range(repeat):
        part = scores[head * BLOCK:(head + 1) * BLOCK] + bias
        highest = jnp.max(part, axis=1, keepdims=True)
        weights.append(jnp.exp2((part - highest) * factor).astype(jnp.bfloat16))
    summed = jnp.dot(
        jnp.concatenate(weights, axis=0), value, preferred_element_type=jnp.float32
    )
    summed = summed[:, :HEAD_SIZE] / summed[:, HEAD_SIZE:]
    for head in range(repeat):
        columns = slice(head * HEAD_SIZE, (head + 1) * HEAD_SIZE)
        out_ref[owner, layer * BLOCK:(layer + 1) * BLOCK, columns] = summed[
            head * BLOCK:(head + 1) * BLOCK
        ].astype(out_ref.dtype)


def differ(one, two, members):
    total, bit = 0, 1
    while bit < members:
        total = total + bit * ((one // bit + two // bit) % 2)
        bit *= 2
    return total


def merge(first, second, one=1, two=1):
    first, second, out = list(first), list(second), []
    while first or second:
        for _ in range(one):
            if first:
                out += first.pop(0)
        for _ in range(two):
            if second:
                out += second.pop(0)
    return out


def after_sends(near_middle, layers):
    pieces = range(PIECES)
    block = range(layers)
    far = [(m, l) for l in block for m in (7, 5, 6, 4)]
    near = [("a", m, l) for l in block for m in (2, 3)]
    out = []
    if near_middle:
        early = [("a", m, l) for m, l in far if m in (4, 5)]
        late = [("a", m, l) for m, l in far if m in (6, 7)]
        out += [("w", 6, p) for p in pieces]
        out += [("a", 1, l) for l in block]
        out += merge([[("w", 4, p)] for p in pieces], [[n] for n in near[:3]])
        out += near[3:]
        out += [("need", 1), ("need", 3), ("P", 0)]
        out += early[:3] + [("P", 2)] + early[3:]
        out += late[:4] + [("P", 4), ("need", 7), ("need", 5), ("Q", 0), ("Q", 2)]
        out += late[4:5] + [("Q", 4)] + late[5:]
    else:
        early = [("a", m, l) for m, l in far if m in (6, 7)]
        late = [("a", m, l) for m, l in far if m in (4, 5)]
        out += [("a", 1, l) for l in block]
        out += near
        out += [("need", 1), ("need", 3), ("P", 0)]
        out += merge([[("w", 4, p)] for p in pieces], [[e] for e in early[:3]])
        out += [("P", 2)]
        out += merge([[("w", 6, p)] for p in pieces], [[e] for e in early[3:]])
        out += late[:4] + [("P", 4)] + late[4:5]
        out += [("need", 5), ("need", 7), ("Q", 0), ("Q", 2), ("Q", 4)] + late[5:]
    out += [("F", l) for l in block]
    return with_relays(out, near_middle, layers)


def with_relays(ops, near_middle, layers):
    turn = 1 if near_middle else 3
    units = [0, 1, 2, 3] + [u ^ turn for u in (4, 5, 6, 7)]
    waiting = [(0, l) for l in range(layers)]
    arrived, out = [], []

    def settle(wanted):
        while any(w in waiting for w in wanted):
            out.append(("x",) + waiting[0])
            arrived.append(waiting.pop(0))
        for w in wanted:
            if w in arrived:
                out.append(("c",) + w)
                arrived.remove(w)

    for op in ops:
        if op[0] == "P":
            settle([(units[u], l) for u in (op[1], op[1] + 1) for l in range(layers)])
        elif op[0] == "F":
            settle([(units[u], op[1]) for u in (6, 7)])
        out.append(op)
        if op[0] == "a":
            waiting.append(op[1:])
            if len(waiting) > LAG:
                out.append(("x",) + waiting[0])
                arrived.append(waiting.pop(0))
    return out


def fused_kernel(
    members, columns, layers,
    queries_hbm, keys_hbm, values_hbm, ids_hbm, count_ref, weight_hbm,
    plan_ref, done_ref,
    queries_ref, keys_ref, values_ref, ids_ref, table_ref, own_ref, spot_ref,
    sent_ref, held_ref, full_ref, acc_ref,
    in_sem, spot_sem, send_n, recv_n, send_a, recv_a,
    send_x, recv_x, send_c, recv_c, send_w, recv_w,
):
    me = lax.axis_index("dp")
    mine = lax.axis_index("mp")
    ring = me // 2
    middle = ((ring + 1) // 2) % 2
    inner = middle == 1
    outer = middle == 0
    half = ring // 2
    owned = weight_hbm.shape[0]
    piece = owned // PIECES
    depth = sent_ref.shape[2]
    reach = columns // 2 * depth

    inputs = [
        pltpu.make_async_copy(ids_hbm, ids_ref, in_sem.at[0]),
        pltpu.make_async_copy(keys_hbm, keys_ref, in_sem.at[1]),
        pltpu.make_async_copy(values_hbm, values_ref, in_sem.at[2]),
        pltpu.make_async_copy(queries_hbm, queries_ref, in_sem.at[3]),
        pltpu.make_async_copy(
            weight_hbm,
            full_ref.at[pl.ds(pl.multiple_of(me * owned, owned), owned)],
            in_sem.at[4],
        ),
    ]
    for copy in inputs:
        copy.start()
    own_ref[...] = jnp.full(own_ref.shape, count_ref[0], jnp.int32)

    barrier = pltpu.get_barrier_semaphore()
    for mask in range(1, members):
        pl.semaphore_signal(
            barrier, inc=1, device_id=(flip(me, mask), mine), device_id_type=MESH
        )
    for mask in (1, 2):
        pl.semaphore_signal(
            barrier, inc=1, device_id=(me, flip(mine, mask)), device_id_type=MESH
        )
    pl.semaphore_wait(barrier, members + 1)

    def remote(src, dst, send, recv, device):
        return pltpu.make_async_remote_copy(
            src_ref=src, dst_ref=dst, send_sem=send, recv_sem=recv,
            device_id=device, device_id_type=MESH,
        )

    def count_copy(mask):
        return remote(
            own_ref, table_ref.at[me], send_n.at[mask], recv_n.at[mask], (flip(me, mask), mine)
        )

    def rows_of(layer):
        return pl.ds(layer * BLOCK, BLOCK)

    def block_copy(mask, layer):
        return remote(
            sent_ref.at[flip(me, mask), rows_of(layer)],
            held_ref.at[mine, me, rows_of(layer)],
            send_a.at[mask, layer], recv_a.at[mask, layer],
            (flip(me, mask), mine),
        )

    def x_copy(mask, layer):
        source = flip(me, mask)
        src = held_ref.at[mine, source, rows_of(layer)]
        if mask == 0:
            src = sent_ref.at[me, rows_of(layer)]
        return remote(
            src, held_ref.at[mine, source, rows_of(layer)],
            send_x.at[mask, layer], recv_x.at[mask, layer],
            (me, flip(mine, 2)),
        )

    def core_copy(mask, layer, far):
        source = flip(me, mask)
        column = flip(mine, 2 * far)
        src = held_ref.at[column, source, rows_of(layer)]
        if mask == 0 and not far:
            src = sent_ref.at[me, rows_of(layer)]
        return remote(
            src, held_ref.at[column, source, rows_of(layer)],
            send_c.at[far, mask, layer], recv_c.at[far, mask, layer],
            (me, flip(mine, 1)),
        )

    def weight_copy(mask, to, part):
        first = pl.multiple_of(flip(me, mask) * owned + part * piece, piece)
        src = full_ref.at[pl.ds(first, piece)]
        if mask == 0:
            src = weight_hbm.at[pl.ds(pl.multiple_of(part * piece, piece), piece)]
        return remote(
            src, full_ref.at[pl.ds(first, piece)],
            send_w.at[mask // 2, to // 2, part], recv_w.at[mask ^ to, part],
            (flip(me, to), mine),
        )

    always, at_inner, at_outer = [], [], []

    def start(kept, make, *where):
        make(*where).start()
        kept.append((make, where))

    for mask in range(1, members):
        start(always, count_copy, mask)

    @pl.when(inner)
    def _():
        for part in range(PIECES):
            start(at_inner, weight_copy, 0, 6, part)

    for part in range(PIECES):
        start(always, weight_copy, 0, 2, part)
    for part in range(PIECES // 2):
        start(always, weight_copy, 0, 1, part)

    table_ref[me] = own_ref[...]
    for mask in range(1, members):
        count_copy(mask).wait_recv()
    lane = lax.broadcasted_iota(jnp.int32, own_ref.shape, 1)
    shift = members.bit_length() - 1
    begin = jnp.zeros(own_ref.shape, jnp.int32)
    first = jnp.zeros(own_ref.shape, jnp.int32)
    slots = jnp.zeros(own_ref.shape, jnp.int32)
    wanted = me + lane * members
    for member in range(members):
        count = table_ref[member]
        first = jnp.where(me == member, begin, first)
        within = wanted - begin
        holds = (within >= 0) & (within < count)
        slots = jnp.where(
            holds, member * layers + lax.shift_right_logical(within, shift), slots
        )
        begin = begin + count
    plan_ref[...] = slots
    table_ref[me] = first
    spot = pltpu.make_async_copy(table_ref.at[me], spot_ref, spot_sem)
    spot.start()
    for copy in inputs[:4]:
        copy.wait()
    spot.wait()
    turn = members * NB - spot_ref[0, 0]

    def attend_for(at):
        owner = differ(me, flip(at, 1), members)
        block = (owner + turn) & (members - 1)
        for layer in range(layers):
            attend_block(
                block + layer * members,
                queries_ref, keys_ref, values_ref, ids_ref, sent_ref, owner, layer,
            )

    @pl.loop(0, 2)
    def _(at):
        attend_for(at)

    for layer in range(layers):
        start(always, block_copy, 1, layer)
        start(always, x_copy, 0, layer)
        start(always, core_copy, 0, layer, 0)
    for part in range(PIECES // 2, PIECES):
        start(always, weight_copy, 0, 1, part)
    held_ref[mine, me] = sent_ref[me]

    @pl.loop(2, 4)
    def _(at):
        attend_for(at)

    for layer in range(layers):
        for mask in (2, 3):
            start(always, block_copy, mask, layer)

    @pl.loop(4, 8)
    def _(at):
        attend_for(at)
        weight_copy(0, 2, at - 4).wait_recv()
        weight_copy(2, 1, at - 4).start()

        @pl.when(inner)
        def _():
            weight_copy(2, 6, at - 4).start()

    always.extend((weight_copy, (2, 1, part)) for part in range(PIECES))
    at_inner.extend((weight_copy, (2, 6, part)) for part in range(PIECES))
    for layer in range(layers):
        for mask in (7, 5, 6, 4):
            start(always, block_copy, mask, layer)
    inputs[4].wait()

    tile = 256
    width = full_ref.shape[1]

    def source_of(at):
        early = (at // 4 + 1) % 2
        far = flip(at, 1) * middle + flip(at, 3) * (1 - middle)
        return differ(me, early * at + (1 - early) * far, members)

    def part_of(which, source, rows, lanes):
        total = None
        for column in range(columns // 2):
            row = pl.multiple_of(which * reach + column * depth, depth)
            part = jnp.dot(
                held_ref[which * (columns // 2) + column, source, rows, :],
                full_ref[pl.ds(row, depth), lanes],
                preferred_element_type=jnp.float32,
            )
            total = part if total is None else total + part
        return total

    every = pl.ds(0, layers * BLOCK)

    def near_product(at):
        source = source_of(at)
        for lane_at in range(0, width, tile):
            lanes = pl.ds(lane_at, tile)
            acc_ref[at, :, lanes] = part_of(half, source, every, lanes)

    def far_product(at):
        source = source_of(at)
        for lane_at in range(0, width, tile):
            lanes = pl.ds(lane_at, tile)
            total = acc_ref[at, :, lanes] + part_of(1 - half, source, every, lanes)
            done_ref[source, :, lanes] = total.astype(done_ref.dtype)

    def whole_product(at, layer):
        source = source_of(at)
        rows = rows_of(layer)
        for lane_at in range(0, width, tile):
            lanes = pl.ds(lane_at, tile)
            total = part_of(half, source, rows, lanes)
            total = total + part_of(1 - half, source, rows, lanes)
            done_ref[source, rows, lanes] = total.astype(done_ref.dtype)

    def product(kind, which):
        if kind == "P":
            pl.loop(which, which + 2)(near_product)
        elif kind == "Q":
            pl.loop(which, which + 2)(far_product)
        else:
            pl.loop(6, 8)(lambda at: whole_product(at, which))

    def step(op, near_middle, kept):
        kind = op[0]
        if kind == "a":
            block_copy(*op[1:]).wait_recv()
            start(kept, x_copy, *op[1:])
            start(kept, core_copy, *op[1:], 0)
        elif kind == "x":
            x_copy(*op[1:]).wait_recv()
            start(kept, core_copy, *op[1:], 1)
        elif kind == "c":
            core_copy(*op[1:], 0).wait_recv()
            core_copy(*op[1:], 1).wait_recv()
        elif kind == "need":
            for part in range(PIECES):
                weight_copy(0, op[1], part).wait_recv()
        elif kind == "w":
            mask, part = op[1:]
            weight_copy(0, mask, part).wait_recv()
            if near_middle:
                start(kept, weight_copy, mask, 2, part)
            start(kept, weight_copy, mask, 1, part)

    plans = [after_sends(True, layers), after_sends(False, layers)]
    while plans[0]:
        stop = None
        for plan, near_middle, kept, here in (
            (plans[0], True, at_inner, inner), (plans[1], False, at_outer, outer)
        ):
            ops = []
            while plan and plan[0][0] not in ("P", "Q", "F"):
                ops.append(plan.pop(0))
            if ops:

                @pl.when(here)
                def _(ops=ops, near_middle=near_middle, kept=kept):
                    for op in ops:
                        step(op, near_middle, kept)

            if plan:
                stop = plan.pop(0)
        if stop is not None:
            product(*stop)

    for kept, here in ((at_inner, inner), (at_outer, outer)):

        @pl.when(here)
        def _(kept=kept):
            for make, where in kept:
                make(*where).wait_send()

    for make, where in always:
        make(*where).wait_send()


def fused(queries, keys, values, ids, live_counts, weight, members, columns, layers):
    anywhere = pl.BlockSpec(memory_space=pl.ANY)
    dma = pltpu.SemaphoreType.DMA
    rows = layers * BLOCK
    depth = queries.shape[2]
    width = weight.shape[1]
    low = jnp.bfloat16
    return pl.pallas_call(
        functools.partial(fused_kernel, members, columns, layers),
        out_shape=(
            pltpu.VMEM((8, 128), jnp.int32),
            pltpu.VMEM((members, rows, width), low),
        ),
        in_specs=[anywhere] * 4 + [pl.BlockSpec(memory_space=pltpu.SMEM), anywhere],
        out_specs=(pl.BlockSpec(memory_space=pltpu.VMEM),) * 2,
        scratch_shapes=[
            pltpu.VMEM(queries.shape, low),
            pltpu.VMEM(keys.shape, low),
            pltpu.VMEM(values.shape, low),
            pltpu.VMEM(ids.shape, jnp.int32),
            pltpu.VMEM((members, 8, 128), jnp.int32),
            pltpu.VMEM((8, 128), jnp.int32),
            pltpu.SMEM((8, 128), jnp.int32),
            pltpu.VMEM((members, rows, depth), low),
            pltpu.VMEM((columns, members, rows, depth), low),
            pltpu.VMEM((members * weight.shape[0], width), low),
            pltpu.VMEM((6, rows, width), jnp.float32),
            dma((5,)),
            dma,
            dma((members,)), dma((members,)),
            dma((members, layers)), dma((members, layers)),
            dma((members, layers)), dma((members, layers)),
            dma((2, members, layers)), dma((2, members, layers)),
            dma((4, 4, PIECES)), dma((members, PIECES)),
        ],
        compiler_params=pltpu.CompilerParams(
            collective_id=2, has_side_effects=True, vmem_limit_bytes=115 * 512 * 1024
        ),
    )(queries, keys, values, ids, live_counts, weight)


def order_kernel(slots_ref, products_ref, out_ref, sem):
    kept = out_ref.shape[0] // BLOCK
    copies = [
        pltpu.make_async_copy(
            products_ref.at[slots_ref[0, at]], out_ref.at[pl.ds(at * BLOCK, BLOCK)], sem.at[at]
        )
        for at in range(kept)
    ]
    for copy in copies:
        copy.start()
    for copy in copies:
        copy.wait()


def in_order(slots, products, kept):
    width = products.shape[2]
    return pl.pallas_call(
        order_kernel,
        out_shape=jax.ShapeDtypeStruct((kept * BLOCK, width), products.dtype),
        in_specs=[
            pl.BlockSpec(memory_space=pltpu.SMEM), pl.BlockSpec(memory_space=pltpu.VMEM)
        ],
        out_specs=pl.BlockSpec(memory_space=pl.ANY),
        scratch_shapes=[pltpu.SemaphoreType.DMA((kept,))],
        compiler_params=pltpu.CompilerParams(vmem_limit_bytes=16 * 1024 * 1024),
    )(slots, products)


def body(members, columns, queries, keys, values, doc_ids, live_counts, out_weight):
    per_owner = (NB + members - 1) // members
    kept = NB * 11 // 12
    half = members // 2
    if members == 8 and columns == 4:
        slots, products = fused(
            queries.reshape(NB, BLOCK, -1), keys.reshape(NB, BLOCK, -1),
            values.reshape(NB, BLOCK, -1), doc_ids.reshape(NB, 1, BLOCK),
            live_counts, out_weight,
            members, columns, per_owner,
        )
        products = products.reshape(members * per_owner, BLOCK, out_weight.shape[1])
        return in_order(slots, products, kept)
    plan = make_plan(live_counts, members, per_owner)
    plan, near_weight = lax.optimization_barrier((plan, out_weight))
    far_weight = lax.ppermute(
        near_weight, "dp", [(i, (i + half) % members) for i in range(members)]
    )
    sent = attend(
        plan, queries, keys, values, doc_ids.reshape(NB, BLOCK), members, per_owner
    )
    held, full = exchange(sent, out_weight, far_weight, members, columns)
    held = held.reshape(columns, members * per_owner, BLOCK, queries.shape[1])
    full = full.reshape(members * out_weight.shape[0], out_weight.shape[1])
    return project(plan, held, full, kept)


def solution(mesh):
    return jax.shard_map(
        functools.partial(body, mesh.shape["dp"], mesh.shape["mp"]),
        mesh=mesh,
        in_specs=(P("dp", "mp"), P("dp", "mp"), P("dp", "mp"), P("dp"), P("dp"), P("dp", "mp")),
        out_specs=P("dp", "mp"),
        check_vma=False,
    )
```

```python
import functools
import math

import jax
import jax.numpy as jnp
from jax import lax
from jax.experimental import pallas as pl
from jax.experimental.pallas import tpu as pltpu
from jax.sharding import PartitionSpec as P

HEAD_SIZE = 128
BLOCK = 128
NB = 24
MESH = pl.DeviceIdType.MESH
MASKED = -1e30
VMEM = 60 * 1024 * 1024


def attend_kernel(per_owner, plan_ref, queries_ref, keys_ref, values_ref, ids_ref, out_ref):
    step = pl.program_id(0)
    repeat = queries_ref.shape[1] // HEAD_SIZE
    factor = math.log2(math.e) / math.sqrt(HEAD_SIZE)
    row_at = lax.broadcasted_iota(jnp.int32, (BLOCK, BLOCK), 0)
    col_at = lax.broadcasted_iota(jnp.int32, (BLOCK, BLOCK), 1)
    causal = col_at <= row_at
    ones = jnp.ones((BLOCK, HEAD_SIZE), jnp.bfloat16)
    for layer in range(per_owner):
        block = plan_ref[0, step * per_owner + layer]
        rows = pl.ds(pl.multiple_of(block * BLOCK, BLOCK), BLOCK)
        along = jnp.broadcast_to(ids_ref[pl.ds(block, 1), :], (BLOCK, BLOCK))
        down = along.T
        bias = jnp.where((along == down) & causal, 0.0, MASKED)
        value = jnp.where(down >= 0, values_ref[rows, :].astype(jnp.float32), 0.0)
        value = jnp.concatenate([value.astype(jnp.bfloat16), ones], axis=1)
        key = keys_ref[rows, :]
        query = queries_ref[rows, :]
        query = jnp.concatenate(
            [query[:, h * HEAD_SIZE:(h + 1) * HEAD_SIZE] for h in range(repeat)], axis=0
        )
        scores = lax.dot_general(
            query, key, (((1,), (1,)), ((), ())), preferred_element_type=jnp.float32
        )
        weights = []
        for head in range(repeat):
            part = scores[head * BLOCK:(head + 1) * BLOCK] + bias
            highest = jnp.max(part, axis=1, keepdims=True)
            weights.append(jnp.exp2((part - highest) * factor).astype(jnp.bfloat16))
        summed = jnp.dot(
            jnp.concatenate(weights, axis=0), value, preferred_element_type=jnp.float32
        )
        summed = summed[:, :HEAD_SIZE] / summed[:, HEAD_SIZE:]
        for head in range(repeat):
            columns = slice(head * HEAD_SIZE, (head + 1) * HEAD_SIZE)
            out_ref[0, layer, :, columns] = summed[head * BLOCK:(head + 1) * BLOCK].astype(
                out_ref.dtype
            )


def attend(plan, queries, keys, values, ids, members, per_owner):
    cols = queries.shape[1]

    def whole(array):
        return pl.BlockSpec(array.shape, lambda i, c: (0, 0))

    return pl.pallas_call(
        functools.partial(attend_kernel, per_owner),
        out_shape=jax.ShapeDtypeStruct((members, per_owner, BLOCK, cols), jnp.bfloat16),
        grid_spec=pltpu.PrefetchScalarGridSpec(
            num_scalar_prefetch=1,
            grid=(members,),
            in_specs=[whole(queries), whole(keys), whole(values), whole(ids)],
            out_specs=pl.BlockSpec((1, per_owner, BLOCK, cols), lambda i, c: (i, 0, 0, 0)),
        ),
        compiler_params=pltpu.CompilerParams(vmem_limit_bytes=VMEM),
        cost_estimate=pl.CostEstimate(
            flops=members * per_owner * cols * BLOCK * BLOCK * 4,
            bytes_accessed=4 * queries.size,
            transcendentals=members * per_owner * cols * BLOCK,
        ),
    )(plan, queries, keys, values, ids)


def flip(index, mask):
    bit = 1
    while bit <= mask:
        if mask & bit:
            index = index + bit - 2 * bit * ((index // bit) % 2)
        bit *= 2
    return index


def plan_kernel(members, per_owner, count_ref, plan_ref, table_ref, send_sem, recv_sem):
    me = lax.axis_index("dp")
    mine = lax.axis_index("mp")
    barrier = pltpu.get_barrier_semaphore()
    for mask in range(1, members):
        pl.semaphore_signal(
            barrier, inc=1, device_id=(flip(me, mask), mine), device_id_type=MESH
        )
    pl.semaphore_wait(barrier, members - 1)
    copies = [
        pltpu.make_async_remote_copy(
            src_ref=count_ref,
            dst_ref=table_ref.at[me],
            send_sem=send_sem.at[mask],
            recv_sem=recv_sem.at[mask],
            device_id=(flip(me, mask), mine),
            device_id_type=MESH,
        )
        for mask in range(1, members)
    ]
    for copy in copies:
        copy.start()
    own_count = count_ref[...]
    table_ref[me] = own_count
    for copy in copies:
        copy.wait()
    row = lax.broadcasted_iota(jnp.int32, own_count.shape, 0)
    lane = lax.broadcasted_iota(jnp.int32, own_count.shape, 1)
    shift = members.bit_length() - 1
    start = jnp.zeros_like(own_count)
    first = jnp.zeros_like(own_count)
    slots = jnp.zeros_like(own_count)
    wanted = me + lane * members
    for member in range(members):
        count = table_ref[member]
        first = jnp.where(me == member, start, first)
        within = wanted - start
        holds = (within >= 0) & (within < count)
        slots = jnp.where(
            holds, member * per_owner + lax.shift_right_logical(within, shift), slots
        )
        start = start + count
    owner = jnp.zeros_like(lane)
    for member in range(1, members):
        owner = owner + (lane >= member * per_owner).astype(jnp.int32)
    layer = lane - owner * per_owner
    turned = (owner - first + members * NB) & (members - 1)
    chosen = jnp.minimum(turned + layer * members, NB - 1)
    chosen = jnp.maximum(chosen, 0)
    plan_ref[...] = jnp.where(row == 0, chosen, slots)


def make_plan(live_counts, members, per_owner):
    count = jnp.broadcast_to(live_counts[:, None], (8, 128))
    dma = pltpu.SemaphoreType.DMA
    return pl.pallas_call(
        functools.partial(plan_kernel, members, per_owner),
        out_shape=jax.ShapeDtypeStruct(count.shape, jnp.int32),
        in_specs=[pl.BlockSpec(memory_space=pltpu.VMEM)],
        out_specs=pl.BlockSpec(memory_space=pltpu.VMEM),
        scratch_shapes=[
            pltpu.VMEM((members,) + count.shape, jnp.int32), dma((members,)), dma((members,))
        ],
        compiler_params=pltpu.CompilerParams(collective_id=1, has_side_effects=True),
    )(count)


def exchange_kernel(
    members, columns, per_owner,
    sent_ref, weight_ref, far_weight_ref, held_ref, full_ref,
    local_sem, send_dp, recv_dp, send_x, recv_x, send_w, recv_w,
):
    me = lax.axis_index("dp")
    mine = lax.axis_index("mp")
    top = members // 2

    def dp_device(mask):
        return (flip(me, mask), mine)

    def mp_device(mask):
        return (me, flip(mine, mask))

    bits = [1 << b for b in reversed(range(columns.bit_length() - 1))]
    barrier = pltpu.get_barrier_semaphore()
    for mask in range(1, members):
        pl.semaphore_signal(barrier, inc=1, device_id=dp_device(mask), device_id_type=MESH)
    for mask in bits:
        pl.semaphore_signal(barrier, inc=1, device_id=mp_device(mask), device_id_type=MESH)
    pl.semaphore_wait(barrier, members - 1 + len(bits))

    def dp_copy(mask, layer, source):
        return pltpu.make_async_remote_copy(
            src_ref=sent_ref.at[flip(me, mask), layer],
            dst_ref=held_ref.at[mine, source, layer],
            send_sem=send_dp.at[mask, layer],
            recv_sem=recv_dp.at[mask, layer],
            device_id=dp_device(mask),
            device_id_type=MESH,
        )

    def mp_copy(place, bit, mask, layer):
        source = flip(me, mask)
        column = flip(mine, place)
        if mask == 0 and place == 0:
            src = sent_ref.at[source, layer]
        else:
            src = held_ref.at[column, source, layer]
        return pltpu.make_async_remote_copy(
            src_ref=src,
            dst_ref=held_ref.at[column, source, layer],
            send_sem=send_x.at[place ^ bit, mask, layer],
            recv_sem=recv_x.at[place ^ bit, mask, layer],
            device_id=mp_device(bit),
            device_id_type=MESH,
        )

    def weight_copy(mask, bit):
        owner = flip(me, mask)
        if mask == 0:
            src = weight_ref
        elif mask == top:
            src = far_weight_ref
        else:
            src = full_ref.at[owner]
        return pltpu.make_async_remote_copy(
            src_ref=src,
            dst_ref=full_ref.at[owner],
            send_sem=send_w.at[mask ^ bit],
            recv_sem=recv_w.at[mask ^ bit],
            device_id=dp_device(bit),
            device_id_type=MESH,
        )

    local = [
        pltpu.make_async_copy(weight_ref, full_ref.at[me], local_sem.at[0]),
        pltpu.make_async_copy(far_weight_ref, full_ref.at[flip(me, top)], local_sem.at[1]),
        pltpu.make_async_copy(sent_ref.at[me], held_ref.at[mine, me], local_sem.at[2]),
    ]
    started = []

    def start(copy):
        copy.start()
        started.append(copy)

    def spread_weight(mask, below):
        bit = below // 2
        while bit >= 1:
            start(weight_copy(mask, bit))
            bit //= 2

    def spread(place, below, mask, layer):
        for bit in bits:
            if bit < below:
                start(mp_copy(place, bit, mask, layer))

    order = sorted(range(1, members), key=lambda t: (-(bin(t).count("1") % 2), t))
    for layer in range(per_owner):
        spread(0, columns, 0, layer)
        for mask in order:
            start(dp_copy(mask, layer, me))
        if layer == 0:
            spread_weight(0, top)
            spread_weight(top, top)
    for copy in local:
        copy.start()

    chunks = [(0, layer) for layer in range(per_owner)]
    chunks += [(mask, layer) for layer in range(per_owner) for mask in order]
    weights = [t for t in range(1, members) if t != top]
    weights.sort(key=lambda t: (-(t & -t), t))
    lag = 3

    def relay(mask, layer):
        for place in range(1, columns):
            lowest = place & -place
            mp_copy(place ^ lowest, lowest, mask, layer).wait_recv()
            spread(place, lowest, mask, layer)

    for at in range(len(chunks) + lag):
        if at < len(chunks):
            mask, layer = chunks[at]
            if mask:
                dp_copy(mask, layer, me).wait_recv()
                spread(0, columns, mask, layer)
        if at >= members and at % 2 and weights:
            arrived = weights.pop(0)
            lowest = arrived & -arrived
            weight_copy(arrived ^ lowest, lowest).wait_recv()
            spread_weight(arrived, lowest)
        if at >= lag:
            relay(*chunks[at - lag])
    for arrived in weights:
        lowest = arrived & -arrived
        weight_copy(arrived ^ lowest, lowest).wait_recv()
        spread_weight(arrived, lowest)
    for copy in started:
        copy.wait_send()
    for copy in local:
        copy.wait()


def exchange(sent, weight, far_weight, members, columns):
    per_owner = sent.shape[1]
    anywhere = pl.BlockSpec(memory_space=pl.ANY)
    dma = pltpu.SemaphoreType.DMA
    return pl.pallas_call(
        functools.partial(exchange_kernel, members, columns, per_owner),
        out_shape=(
            jax.ShapeDtypeStruct((columns,) + sent.shape, sent.dtype),
            jax.ShapeDtypeStruct((members,) + weight.shape, weight.dtype),
        ),
        in_specs=[anywhere] * 3,
        out_specs=(anywhere, anywhere),
        scratch_shapes=[
            dma((3,)),
            dma((members, per_owner)),
            dma((members, per_owner)),
            dma((columns, members, per_owner)),
            dma((columns, members, per_owner)),
            dma((members,)),
            dma((members,)),
        ],
        compiler_params=pltpu.CompilerParams(collective_id=0, has_side_effects=True, vmem_limit_bytes=VMEM),
        cost_estimate=pl.CostEstimate(
            flops=0, bytes_accessed=60 * sent.size, transcendentals=0
        ),
    )(sent, weight, far_weight)


def project_kernel(columns, slots_ref, first_ref, second_ref, weight_ref, out_ref):
    total = None
    for column in range(columns):
        rows = jnp.concatenate([first_ref[column, 0], second_ref[column, 0]], axis=0)
        depth = rows.shape[1]
        part = jnp.dot(
            rows, weight_ref[column * depth:(column + 1) * depth, :],
            preferred_element_type=jnp.float32,
        )
        total = part if total is None else total + part
    out_ref[...] = total.astype(out_ref.dtype)


def project(slots, held, weight, kept):
    columns, total, _, depth = held.shape
    width = weight.shape[1]

    def picked(which):
        return pl.BlockSpec(
            (columns, 1, BLOCK, depth), lambda i, s: (0, s[1, 2 * i + which], 0, 0)
        )

    return pl.pallas_call(
        functools.partial(project_kernel, columns),
        out_shape=jax.ShapeDtypeStruct((kept * BLOCK, width), jnp.bfloat16),
        grid_spec=pltpu.PrefetchScalarGridSpec(
            num_scalar_prefetch=1,
            grid=(kept // 2,),
            in_specs=[
                picked(0),
                picked(1),
                pl.BlockSpec(weight.shape, lambda i, s: (0, 0)),
            ],
            out_specs=pl.BlockSpec((2 * BLOCK, width), lambda i, s: (i, 0)),
        ),
        compiler_params=pltpu.CompilerParams(vmem_limit_bytes=VMEM),
    )(slots, held, held, weight)


PIECES = 4
LAG = 3


def attend_block(block, queries_ref, keys_ref, values_ref, ids_ref, out_ref, owner, layer):
    repeat = queries_ref.shape[2] // HEAD_SIZE
    factor = math.log2(math.e) / math.sqrt(HEAD_SIZE)
    row_at = lax.broadcasted_iota(jnp.int32, (BLOCK, BLOCK), 0)
    col_at = lax.broadcasted_iota(jnp.int32, (BLOCK, BLOCK), 1)
    ones = jnp.ones((BLOCK, HEAD_SIZE), jnp.bfloat16)
    along = jnp.broadcast_to(ids_ref[block], (BLOCK, BLOCK))
    down = along.T
    bias = jnp.where((along == down) & (col_at <= row_at), 0.0, MASKED)
    value = jnp.where(down >= 0, values_ref[block].astype(jnp.float32), 0.0)
    value = jnp.concatenate([value.astype(jnp.bfloat16), ones], axis=1)
    key = keys_ref[block]
    query = queries_ref[block]
    query = jnp.concatenate(
        [query[:, h * HEAD_SIZE:(h + 1) * HEAD_SIZE] for h in range(repeat)], axis=0
    )
    scores = lax.dot_general(
        query, key, (((1,), (1,)), ((), ())), preferred_element_type=jnp.float32
    )
    weights = []
    for head in range(repeat):
        part = scores[head * BLOCK:(head + 1) * BLOCK] + bias
        highest = jnp.max(part, axis=1, keepdims=True)
        weights.append(jnp.exp2((part - highest) * factor).astype(jnp.bfloat16))
    summed = jnp.dot(
        jnp.concatenate(weights, axis=0), value, preferred_element_type=jnp.float32
    )
    summed = summed[:, :HEAD_SIZE] / summed[:, HEAD_SIZE:]
    for head in range(repeat):
        columns = slice(head * HEAD_SIZE, (head + 1) * HEAD_SIZE)
        out_ref[owner, layer * BLOCK:(layer + 1) * BLOCK, columns] = summed[
            head * BLOCK:(head + 1) * BLOCK
        ].astype(out_ref.dtype)


def differ(one, two, members):
    total, bit = 0, 1
    while bit < members:
        total = total + bit * ((one // bit + two // bit) % 2)
        bit *= 2
    return total


def merge(first, second, one=1, two=1):
    first, second, out = list(first), list(second), []
    while first or second:
        for _ in range(one):
            if first:
                out += first.pop(0)
        for _ in range(two):
            if second:
                out += second.pop(0)
    return out


def far_order(layers):
    order = [(m, l) for l in range(layers - 1) for m in (7, 5, 6, 4)]
    return order + [(m, layers - 1) for m in (5, 4, 7, 6)]


def after_sends(near_middle, layers):
    pieces = range(PIECES)
    block = range(layers)
    far = far_order(layers)
    near = [("a", m, l) for l in block for m in (2, 3)]
    out = []
    if near_middle:
        early = [("a", m, l) for m, l in far if m in (4, 5)]
        late = [("a", m, l) for m, l in far if m in (6, 7)]
        out += [("w", 6, p) for p in pieces]
        out += [("a", 1, l) for l in block]
        out += merge([[("w", 4, p)] for p in pieces], [[n] for n in near[:3]])
        out += near[3:] + early[:4]
        out += [("need", 1), ("need", 3), ("P", 0, 2)] + early[4:5] + [("P", 2, 2)] + early[5:]
        out += late[:1] + [("need", 7), ("R", 0, 2), ("R", 2, 2)] + late[1:2]
        out += [("P", 4, 1), ("P", 5, 1), ("R", 4, 2)] + late[2:4]
        out += [("need", 5), ("Q", 0, 2), ("Q", 2, 2), ("Q", 4, 2), ("keep", 0)]
        out += [("F", 0), ("F", 1), late[4], late[5], ("G", 6), ("G", 7)]
    else:
        early = [("a", m, l) for m, l in far if m in (6, 7)]
        late = [("a", m, l) for m, l in far if m in (4, 5)]
        weights = [("w", 6, p) for p in pieces]
        out += [("a", 1, l) for l in block]
        out += near
        out += merge([[("w", 4, p)] for p in pieces], [[e] for e in early[:3]])
        out += [("need", 1), ("need", 3), ("P", 0, 2)]
        out += [weights[0], late[0], early[3], ("P", 2, 2), late[1], weights[1], early[4]]
        out += [("need", 5), ("R", 0, 2), late[2], weights[2], early[5], ("R", 2, 2), ("P", 4, 1)]
        out += [weights[3], ("keep", 1), late[3], ("keep", 1), ("P", 5, 1), late[4], ("R", 4, 2)]
        out += [("need", 7), ("Q", 0, 2), late[5], ("Q", 2, 2), ("Q", 4, 2)]
        out += [("F", 0), ("F", 1), ("G", 6), ("G", 7)]
    return with_relays(out, near_middle, layers)


def units_of(near_middle):
    turn = 1 if near_middle else 3
    return [0, 1, 2, 3] + [u ^ turn for u in (4, 5, 6, 7)]


def with_relays(ops, near_middle, layers):
    units = units_of(near_middle)
    waiting = [(0, l) for l in range(layers)]
    out = []

    def settle(left):
        while len(waiting) > left:
            out.append(("x",) + waiting.pop(0))

    for op in ops:
        if op[0] == "keep":
            settle(op[1])
            continue
        if op[0] in ("P", "F", "G"):
            which = range(op[1], op[1] + op[2]) if op[0] == "P" else (6, 7)
            which = op[1:] if op[0] == "G" else which
            rows = {"P": range(layers), "F": op[1:2], "G": [layers - 1]}[op[0]]
            wanted = [(units[u], l) for u in which for l in rows]
            while any(w in waiting for w in wanted):
                settle(len(waiting) - 1)
            out.extend([("c", op[0], u) for u in which] if op[0] != "F" else [("c",) + op])
        out.append(op)
        if op[0] == "a":
            waiting.append(op[1:])
            settle(LAG)
    return out


def fused_kernel(
    members, columns, layers,
    queries_hbm, keys_hbm, values_hbm, ids_hbm, count_ref, weight_hbm,
    plan_ref, done_ref,
    queries_ref, keys_ref, values_ref, ids_ref, table_ref, own_ref, spot_ref,
    sent_ref, held_ref, full_ref, acc_ref,
    in_sem, spot_sem, send_n, recv_n, send_a, recv_a,
    send_x, recv_x, send_c, recv_c, send_w, recv_w, recv_y,
):
    me = lax.axis_index("dp")
    mine = lax.axis_index("mp")
    ring = me // 2
    middle = ((ring + 1) // 2) % 2
    inner = middle == 1
    outer = middle == 0
    half = ring // 2
    owned = weight_hbm.shape[0]
    piece = owned // PIECES
    depth = sent_ref.shape[2]
    reach = columns // 2 * depth

    inputs = [
        pltpu.make_async_copy(ids_hbm, ids_ref, in_sem.at[0]),
        pltpu.make_async_copy(keys_hbm, keys_ref, in_sem.at[1]),
        pltpu.make_async_copy(values_hbm, values_ref, in_sem.at[2]),
        pltpu.make_async_copy(queries_hbm, queries_ref, in_sem.at[3]),
        pltpu.make_async_copy(
            weight_hbm,
            full_ref.at[pl.ds(pl.multiple_of(me * owned, owned), owned)],
            in_sem.at[4],
        ),
    ]
    for copy in inputs:
        copy.start()
    own_ref[...] = jnp.full(own_ref.shape, count_ref[0], jnp.int32)

    barrier = pltpu.get_barrier_semaphore()
    for mask in range(1, members):
        pl.semaphore_signal(
            barrier, inc=1, device_id=(flip(me, mask), mine), device_id_type=MESH
        )
    for mask in (1, 2):
        pl.semaphore_signal(
            barrier, inc=1, device_id=(me, flip(mine, mask)), device_id_type=MESH
        )
    pl.semaphore_wait(barrier, members + 1)

    def remote(src, dst, send, recv, device):
        return pltpu.make_async_remote_copy(
            src_ref=src, dst_ref=dst, send_sem=send, recv_sem=recv,
            device_id=device, device_id_type=MESH,
        )

    def count_copy(mask):
        return remote(
            own_ref, table_ref.at[me], send_n, recv_n, (flip(me, mask), mine)
        )

    def rows_of(layer):
        return pl.ds(layer * BLOCK, BLOCK)

    def block_copy(mask, layer):
        return remote(
            sent_ref.at[flip(me, mask), rows_of(layer)],
            held_ref.at[mine, me, rows_of(layer)],
            send_a, recv_a.at[mask, layer],
            (flip(me, mask), mine),
        )

    def x_copy(mask, layer):
        source = flip(me, mask)
        src = held_ref.at[mine, source, rows_of(layer)]
        if mask == 0:
            src = sent_ref.at[me, rows_of(layer)]
        return remote(
            src, held_ref.at[mine, source, rows_of(layer)],
            send_x, recv_x.at[mask, layer],
            (me, flip(mine, 2)),
        )

    def core_sem(unit, layer):
        if unit < 6:
            return unit
        return 6 + layer + (unit - 6) * (layer // (layers - 1))

    def core_copy(unit, mask, layer, far):
        source = flip(me, mask)
        column = flip(mine, 2 * far)
        src = held_ref.at[column, source, rows_of(layer)]
        if mask == 0 and not far:
            src = sent_ref.at[me, rows_of(layer)]
        return remote(
            src, held_ref.at[column, source, rows_of(layer)],
            send_c, recv_c.at[core_sem(unit, layer)],
            (me, flip(mine, 1)),
        )

    def weight_copy(mask, to, part):
        first = pl.multiple_of(flip(me, mask) * owned + part * piece, piece)
        src = full_ref.at[pl.ds(first, piece)]
        if mask == 0:
            src = weight_hbm.at[pl.ds(pl.multiple_of(part * piece, piece), piece)]
        return remote(
            src, full_ref.at[pl.ds(first, piece)],
            send_w, recv_w.at[mask ^ to, part] if to > 1 else recv_y.at[mask // 2],
            (flip(me, to), mine),
        )

    def landed(bytes_of, sem):
        pltpu.make_async_copy(bytes_of, bytes_of, sem).wait()

    def start(make, *where):
        make(*where).start()

    for mask in range(1, members):
        start(count_copy, mask)

    @pl.when(inner)
    def _():
        for part in range(PIECES):
            start(weight_copy, 0, 6, part)

    for part in range(PIECES):
        start(weight_copy, 0, 2, part)
    for part in range(PIECES // 2):
        start(weight_copy, 0, 1, part)

    table_ref[me] = own_ref[...]
    landed(table_ref.at[pl.ds(0, members - 1)], recv_n)
    lane = lax.broadcasted_iota(jnp.int32, own_ref.shape, 1)
    shift = members.bit_length() - 1
    begin = jnp.zeros(own_ref.shape, jnp.int32)
    first = jnp.zeros(own_ref.shape, jnp.int32)
    slots = jnp.zeros(own_ref.shape, jnp.int32)
    wanted = me + lane * members
    for member in range(members):
        count = table_ref[member]
        first = jnp.where(me == member, begin, first)
        within = wanted - begin
        holds = (within >= 0) & (within < count)
        slots = jnp.where(
            holds, member * layers + lax.shift_right_logical(within, shift), slots
        )
        begin = begin + count
    plan_ref[...] = slots
    table_ref[me] = first
    spot = pltpu.make_async_copy(table_ref.at[me], spot_ref, spot_sem)
    spot.start()
    for copy in inputs[:4]:
        copy.wait()
    spot.wait()
    turn = members * NB - spot_ref[0, 0]

    def attend_for(at):
        owner = differ(me, flip(at, 1), members)
        block = (owner + turn) & (members - 1)
        for layer in range(layers):
            attend_block(
                block + layer * members,
                queries_ref, keys_ref, values_ref, ids_ref, sent_ref, owner, layer,
            )

    @pl.loop(0, 2)
    def _(at):
        attend_for(at)

    for layer in range(layers):
        start(block_copy, 1, layer)
        start(x_copy, 0, layer)
        start(core_copy, 0, 0, layer, 0)
    for part in range(PIECES // 2, PIECES):
        start(weight_copy, 0, 1, part)
    held_ref[mine, me] = sent_ref[me]

    @pl.loop(2, 4)
    def _(at):
        attend_for(at)

    for layer in range(layers):
        for mask in (2, 3):
            start(block_copy, mask, layer)

    @pl.loop(4, 8)
    def _(at):
        attend_for(at)
        weight_copy(0, 2, at - 4).wait_recv()
        weight_copy(2, 1, at - 4).start()

        @pl.when(inner)
        def _():
            weight_copy(2, 6, at - 4).start()

    for mask, layer in far_order(layers):
        start(block_copy, mask, layer)
    inputs[4].wait()

    tile = 256
    width = full_ref.shape[1]

    def source_of(at):
        early = (at // 4 + 1) % 2
        far = flip(at, 1) * middle + flip(at, 3) * (1 - middle)
        return differ(me, early * at + (1 - early) * far, members)

    def part_of(column, source, rows, lanes):
        return jnp.dot(
            held_ref[column, source, rows, :],
            full_ref[pl.ds(pl.multiple_of(column * depth, depth), depth), lanes],
            preferred_element_type=jnp.float32,
        )

    every = pl.ds(0, layers * BLOCK)
    sooner = flip(ring, 3) * middle + flip(ring, 2) * (1 - middle)
    later = flip(ring, 2) * middle + flip(ring, 3) * (1 - middle)

    def near_product(at):
        source = source_of(at)
        for lane_at in range(0, width, tile):
            lanes = pl.ds(lane_at, tile)
            total = part_of(ring, source, every, lanes)
            acc_ref[at, :, lanes] = total + part_of(flip(ring, 1), source, every, lanes)

    def sooner_product(at):
        source = source_of(at)
        for lane_at in range(0, width, tile):
            lanes = pl.ds(lane_at, tile)
            acc_ref[at, :, lanes] += part_of(sooner, source, every, lanes)

    def later_product(at):
        source = source_of(at)
        for lane_at in range(0, width, tile):
            lanes = pl.ds(lane_at, tile)
            total = acc_ref[at, :, lanes] + part_of(later, source, every, lanes)
            done_ref[source, :, lanes] = total.astype(done_ref.dtype)

    def whole_product(layer):
        rows = rows_of(layer)
        one, two = source_of(6), source_of(7)
        for lane_at in range(0, width, tile):
            lanes = pl.ds(lane_at, tile)
            total = None
            for column in range(columns):
                part = jnp.dot(
                    jnp.concatenate(
                        [held_ref[column, one, rows, :], held_ref[column, two, rows, :]], axis=0
                    ),
                    full_ref[pl.ds(column * depth, depth), lanes],
                    preferred_element_type=jnp.float32,
                )
                total = part if total is None else total + part
            total = total.astype(done_ref.dtype)
            done_ref[one, rows, lanes] = total[:BLOCK]
            done_ref[two, rows, lanes] = total[BLOCK:]

    def last_product(at):
        source = source_of(at)
        rows = rows_of(layers - 1)
        for lane_at in range(0, width, tile):
            lanes = pl.ds(lane_at, tile)
            total = None
            for column in range(columns):
                part = part_of(column, source, rows, lanes)
                total = part if total is None else total + part
            done_ref[source, rows, lanes] = total.astype(done_ref.dtype)

    def product(kind, which, count=1):
        if kind == "F":
            whole_product(which)
        elif kind == "G":
            last_product(which)
        else:
            one = {"P": near_product, "R": sooner_product, "Q": later_product}[kind]
            pl.loop(which, which + count)(one)

    def step(op, near_middle):
        kind = op[0]
        units = units_of(near_middle)
        if kind == "a":
            block_copy(*op[1:]).wait_recv()
            start(x_copy, *op[1:])
            start(core_copy, units.index(op[1]), *op[1:], 0)
        elif kind == "x":
            x_copy(*op[1:]).wait_recv()
            start(core_copy, units.index(op[1]), *op[1:], 1)
        elif kind == "c" and op[1] == "P":
            landed(held_ref.at[pl.ds(0, 2), 0], recv_c.at[op[2]])
        elif kind == "c" and op[1] == "F":
            landed(held_ref.at[pl.ds(0, 4), 0, rows_of(op[2])], recv_c.at[6 + op[2]])
        elif kind == "c":
            landed(
                held_ref.at[pl.ds(0, 2), 0, rows_of(layers - 1)],
                recv_c.at[core_sem(op[2], layers - 1)],
            )
        elif kind == "need":
            first = pl.multiple_of(flip(me, op[1]) * owned, owned)
            landed(full_ref.at[pl.ds(first, owned)], recv_y.at[op[1] // 2])
        elif kind == "w":
            mask, part = op[1:]
            weight_copy(0, mask, part).wait_recv()
            if near_middle:
                start(weight_copy, mask, 2, part)
            start(weight_copy, mask, 1, part)

    plans = [after_sends(True, layers), after_sends(False, layers)]
    while plans[0]:
        stop = None
        for plan, near_middle, here in ((plans[0], True, inner), (plans[1], False, outer)):
            ops = []
            while plan and plan[0][0] not in ("P", "R", "Q", "F", "G"):
                ops.append(plan.pop(0))
            if ops:

                @pl.when(here)
                def _(ops=ops, near_middle=near_middle):
                    for op in ops:
                        step(op, near_middle)

            stop = plan.pop(0)
        product(*stop)

    landed(table_ref.at[pl.ds(0, members - 1)], send_n)
    landed(sent_ref.at[pl.ds(0, members - 1)], send_a)
    landed(sent_ref, send_x)
    landed(held_ref.at[pl.ds(0, 2)], send_c)

    @pl.when(inner)
    def _():
        landed(held_ref.at[pl.ds(0, 4), pl.ds(0, 3)], send_w)

    @pl.when(outer)
    def _():
        landed(full_ref.at[pl.ds(0, 5 * PIECES * piece)], send_w)


def fused(queries, keys, values, ids, live_counts, weight, members, columns, layers):
    anywhere = pl.BlockSpec(memory_space=pl.ANY)
    dma = pltpu.SemaphoreType.DMA
    rows = layers * BLOCK
    depth = queries.shape[2]
    width = weight.shape[1]
    low = jnp.bfloat16
    return pl.pallas_call(
        functools.partial(fused_kernel, members, columns, layers),
        out_shape=(
            pltpu.VMEM((8, 128), jnp.int32),
            pltpu.VMEM((members, rows, width), low),
        ),
        in_specs=[anywhere] * 4 + [pl.BlockSpec(memory_space=pltpu.SMEM), anywhere],
        out_specs=(pl.BlockSpec(memory_space=pltpu.VMEM),) * 2,
        scratch_shapes=[
            pltpu.VMEM(queries.shape, low),
            pltpu.VMEM(keys.shape, low),
            pltpu.VMEM(values.shape, low),
            pltpu.VMEM(ids.shape, jnp.int32),
            pltpu.VMEM((members, 8, 128), jnp.int32),
            pltpu.VMEM((8, 128), jnp.int32),
            pltpu.SMEM((8, 128), jnp.int32),
            pltpu.VMEM((members, rows, depth), low),
            pltpu.VMEM((columns, members, rows, depth), low),
            pltpu.VMEM((members * weight.shape[0], width), low),
            pltpu.VMEM((6, rows, width), jnp.float32),
            dma((5,)),
            dma,
            dma, dma,
            dma, dma((members, layers)),
            dma, dma((members, layers)),
            dma, dma((7 + layers,)),
            dma, dma((members, PIECES)), dma((4,)),
        ],
        compiler_params=pltpu.CompilerParams(
            collective_id=2, has_side_effects=True, vmem_limit_bytes=115 * 512 * 1024
        ),
    )(queries, keys, values, ids, live_counts, weight)


def order_kernel(slots_ref, products_ref, out_ref, sem):
    kept = out_ref.shape[0] // BLOCK
    copies = [
        pltpu.make_async_copy(
            products_ref.at[slots_ref[0, at]], out_ref.at[pl.ds(at * BLOCK, BLOCK)], sem.at[at]
        )
        for at in range(kept)
    ]
    for copy in copies:
        copy.start()
    for copy in copies:
        copy.wait()


def in_order(slots, products, kept):
    width = products.shape[2]
    return pl.pallas_call(
        order_kernel,
        out_shape=jax.ShapeDtypeStruct((kept * BLOCK, width), products.dtype),
        in_specs=[
            pl.BlockSpec(memory_space=pltpu.SMEM), pl.BlockSpec(memory_space=pltpu.VMEM)
        ],
        out_specs=pl.BlockSpec(memory_space=pl.ANY),
        scratch_shapes=[pltpu.SemaphoreType.DMA((kept,))],
        compiler_params=pltpu.CompilerParams(vmem_limit_bytes=16 * 1024 * 1024),
    )(slots, products)


def body(members, columns, queries, keys, values, doc_ids, live_counts, out_weight):
    per_owner = (NB + members - 1) // members
    kept = NB * 11 // 12
    half = members // 2
    if members == 8 and columns == 4:
        slots, products = fused(
            queries.reshape(NB, BLOCK, -1), keys.reshape(NB, BLOCK, -1),
            values.reshape(NB, BLOCK, -1), doc_ids.reshape(NB, 1, BLOCK),
            live_counts, out_weight,
            members, columns, per_owner,
        )
        products = products.reshape(members * per_owner, BLOCK, out_weight.shape[1])
        return in_order(slots, products, kept)
    plan = make_plan(live_counts, members, per_owner)
    plan, near_weight = lax.optimization_barrier((plan, out_weight))
    far_weight = lax.ppermute(
        near_weight, "dp", [(i, (i + half) % members) for i in range(members)]
    )
    sent = attend(
        plan, queries, keys, values, doc_ids.reshape(NB, BLOCK), members, per_owner
    )
    held, full = exchange(sent, out_weight, far_weight, members, columns)
    held = held.reshape(columns, members * per_owner, BLOCK, queries.shape[1])
    full = full.reshape(members * out_weight.shape[0], out_weight.shape[1])
    return project(plan, held, full, kept)


def solution(mesh):
    return jax.shard_map(
        functools.partial(body, mesh.shape["dp"], mesh.shape["mp"]),
        mesh=mesh,
        in_specs=(P("dp", "mp"), P("dp", "mp"), P("dp", "mp"), P("dp"), P("dp"), P("dp", "mp")),
        out_specs=P("dp", "mp"),
        check_vma=False,
    )
```

```python
import functools
import math

import jax
import jax.numpy as jnp
from jax import lax
from jax.experimental import pallas as pl
from jax.experimental.pallas import tpu as pltpu
from jax.sharding import PartitionSpec as P

HEAD_SIZE = 128
BLOCK = 128
NB = 24
MESH = pl.DeviceIdType.MESH
MASKED = -1e30
VMEM = 60 * 1024 * 1024


def attend_kernel(per_owner, plan_ref, queries_ref, keys_ref, values_ref, ids_ref, out_ref):
    step = pl.program_id(0)
    repeat = queries_ref.shape[1] // HEAD_SIZE
    factor = math.log2(math.e) / math.sqrt(HEAD_SIZE)
    row_at = lax.broadcasted_iota(jnp.int32, (BLOCK, BLOCK), 0)
    col_at = lax.broadcasted_iota(jnp.int32, (BLOCK, BLOCK), 1)
    causal = col_at <= row_at
    ones = jnp.ones((BLOCK, HEAD_SIZE), jnp.bfloat16)
    for layer in range(per_owner):
        block = plan_ref[0, step * per_owner + layer]
        rows = pl.ds(pl.multiple_of(block * BLOCK, BLOCK), BLOCK)
        along = jnp.broadcast_to(ids_ref[pl.ds(block, 1), :], (BLOCK, BLOCK))
        down = along.T
        bias = jnp.where((along == down) & causal, 0.0, MASKED)
        value = jnp.where(down >= 0, values_ref[rows, :].astype(jnp.float32), 0.0)
        value = jnp.concatenate([value.astype(jnp.bfloat16), ones], axis=1)
        key = keys_ref[rows, :]
        query = queries_ref[rows, :]
        query = jnp.concatenate(
            [query[:, h * HEAD_SIZE:(h + 1) * HEAD_SIZE] for h in range(repeat)], axis=0
        )
        scores = lax.dot_general(
            query, key, (((1,), (1,)), ((), ())), preferred_element_type=jnp.float32
        )
        weights = []
        for head in range(repeat):
            part = scores[head * BLOCK:(head + 1) * BLOCK] + bias
            highest = jnp.max(part, axis=1, keepdims=True)
            weights.append(jnp.exp2((part - highest) * factor).astype(jnp.bfloat16))
        summed = jnp.dot(
            jnp.concatenate(weights, axis=0), value, preferred_element_type=jnp.float32
        )
        summed = summed[:, :HEAD_SIZE] / summed[:, HEAD_SIZE:]
        for head in range(repeat):
            columns = slice(head * HEAD_SIZE, (head + 1) * HEAD_SIZE)
            out_ref[0, layer, :, columns] = summed[head * BLOCK:(head + 1) * BLOCK].astype(
                out_ref.dtype
            )


def attend(plan, queries, keys, values, ids, members, per_owner):
    cols = queries.shape[1]

    def whole(array):
        return pl.BlockSpec(array.shape, lambda i, c: (0, 0))

    return pl.pallas_call(
        functools.partial(attend_kernel, per_owner),
        out_shape=jax.ShapeDtypeStruct((members, per_owner, BLOCK, cols), jnp.bfloat16),
        grid_spec=pltpu.PrefetchScalarGridSpec(
            num_scalar_prefetch=1,
            grid=(members,),
            in_specs=[whole(queries), whole(keys), whole(values), whole(ids)],
            out_specs=pl.BlockSpec((1, per_owner, BLOCK, cols), lambda i, c: (i, 0, 0, 0)),
        ),
        compiler_params=pltpu.CompilerParams(vmem_limit_bytes=VMEM),
        cost_estimate=pl.CostEstimate(
            flops=members * per_owner * cols * BLOCK * BLOCK * 4,
            bytes_accessed=4 * queries.size,
            transcendentals=members * per_owner * cols * BLOCK,
        ),
    )(plan, queries, keys, values, ids)


def flip(index, mask):
    bit = 1
    while bit <= mask:
        if mask & bit:
            index = index + bit - 2 * bit * ((index // bit) % 2)
        bit *= 2
    return index


def plan_kernel(members, per_owner, count_ref, plan_ref, table_ref, send_sem, recv_sem):
    me = lax.axis_index("dp")
    mine = lax.axis_index("mp")
    barrier = pltpu.get_barrier_semaphore()
    for mask in range(1, members):
        pl.semaphore_signal(
            barrier, inc=1, device_id=(flip(me, mask), mine), device_id_type=MESH
        )
    pl.semaphore_wait(barrier, members - 1)
    copies = [
        pltpu.make_async_remote_copy(
            src_ref=count_ref,
            dst_ref=table_ref.at[me],
            send_sem=send_sem.at[mask],
            recv_sem=recv_sem.at[mask],
            device_id=(flip(me, mask), mine),
            device_id_type=MESH,
        )
        for mask in range(1, members)
    ]
    for copy in copies:
        copy.start()
    own_count = count_ref[...]
    table_ref[me] = own_count
    for copy in copies:
        copy.wait()
    row = lax.broadcasted_iota(jnp.int32, own_count.shape, 0)
    lane = lax.broadcasted_iota(jnp.int32, own_count.shape, 1)
    shift = members.bit_length() - 1
    start = jnp.zeros_like(own_count)
    first = jnp.zeros_like(own_count)
    slots = jnp.zeros_like(own_count)
    wanted = me + lane * members
    for member in range(members):
        count = table_ref[member]
        first = jnp.where(me == member, start, first)
        within = wanted - start
        holds = (within >= 0) & (within < count)
        slots = jnp.where(
            holds, member * per_owner + lax.shift_right_logical(within, shift), slots
        )
        start = start + count
    owner = jnp.zeros_like(lane)
    for member in range(1, members):
        owner = owner + (lane >= member * per_owner).astype(jnp.int32)
    layer = lane - owner * per_owner
    turned = (owner - first + members * NB) & (members - 1)
    chosen = jnp.minimum(turned + layer * members, NB - 1)
    chosen = jnp.maximum(chosen, 0)
    plan_ref[...] = jnp.where(row == 0, chosen, slots)


def make_plan(live_counts, members, per_owner):
    count = jnp.broadcast_to(live_counts[:, None], (8, 128))
    dma = pltpu.SemaphoreType.DMA
    return pl.pallas_call(
        functools.partial(plan_kernel, members, per_owner),
        out_shape=jax.ShapeDtypeStruct(count.shape, jnp.int32),
        in_specs=[pl.BlockSpec(memory_space=pltpu.VMEM)],
        out_specs=pl.BlockSpec(memory_space=pltpu.VMEM),
        scratch_shapes=[
            pltpu.VMEM((members,) + count.shape, jnp.int32), dma((members,)), dma((members,))
        ],
        compiler_params=pltpu.CompilerParams(collective_id=1, has_side_effects=True),
    )(count)


def exchange_kernel(
    members, columns, per_owner,
    sent_ref, weight_ref, far_weight_ref, held_ref, full_ref,
    local_sem, send_dp, recv_dp, send_x, recv_x, send_w, recv_w,
):
    me = lax.axis_index("dp")
    mine = lax.axis_index("mp")
    top = members // 2

    def dp_device(mask):
        return (flip(me, mask), mine)

    def mp_device(mask):
        return (me, flip(mine, mask))

    bits = [1 << b for b in reversed(range(columns.bit_length() - 1))]
    barrier = pltpu.get_barrier_semaphore()
    for mask in range(1, members):
        pl.semaphore_signal(barrier, inc=1, device_id=dp_device(mask), device_id_type=MESH)
    for mask in bits:
        pl.semaphore_signal(barrier, inc=1, device_id=mp_device(mask), device_id_type=MESH)
    pl.semaphore_wait(barrier, members - 1 + len(bits))

    def dp_copy(mask, layer, source):
        return pltpu.make_async_remote_copy(
            src_ref=sent_ref.at[flip(me, mask), layer],
            dst_ref=held_ref.at[mine, source, layer],
            send_sem=send_dp.at[mask, layer],
            recv_sem=recv_dp.at[mask, layer],
            device_id=dp_device(mask),
            device_id_type=MESH,
        )

    def mp_copy(place, bit, mask, layer):
        source = flip(me, mask)
        column = flip(mine, place)
        if mask == 0 and place == 0:
            src = sent_ref.at[source, layer]
        else:
            src = held_ref.at[column, source, layer]
        return pltpu.make_async_remote_copy(
            src_ref=src,
            dst_ref=held_ref.at[column, source, layer],
            send_sem=send_x.at[place ^ bit, mask, layer],
            recv_sem=recv_x.at[place ^ bit, mask, layer],
            device_id=mp_device(bit),
            device_id_type=MESH,
        )

    def weight_copy(mask, bit):
        owner = flip(me, mask)
        if mask == 0:
            src = weight_ref
        elif mask == top:
            src = far_weight_ref
        else:
            src = full_ref.at[owner]
        return pltpu.make_async_remote_copy(
            src_ref=src,
            dst_ref=full_ref.at[owner],
            send_sem=send_w.at[mask ^ bit],
            recv_sem=recv_w.at[mask ^ bit],
            device_id=dp_device(bit),
            device_id_type=MESH,
        )

    local = [
        pltpu.make_async_copy(weight_ref, full_ref.at[me], local_sem.at[0]),
        pltpu.make_async_copy(far_weight_ref, full_ref.at[flip(me, top)], local_sem.at[1]),
        pltpu.make_async_copy(sent_ref.at[me], held_ref.at[mine, me], local_sem.at[2]),
    ]
    started = []

    def start(copy):
        copy.start()
        started.append(copy)

    def spread_weight(mask, below):
        bit = below // 2
        while bit >= 1:
            start(weight_copy(mask, bit))
            bit //= 2

    def spread(place, below, mask, layer):
        for bit in bits:
            if bit < below:
                start(mp_copy(place, bit, mask, layer))

    order = sorted(range(1, members), key=lambda t: (-(bin(t).count("1") % 2), t))
    for layer in range(per_owner):
        spread(0, columns, 0, layer)
        for mask in order:
            start(dp_copy(mask, layer, me))
        if layer == 0:
            spread_weight(0, top)
            spread_weight(top, top)
    for copy in local:
        copy.start()

    chunks = [(0, layer) for layer in range(per_owner)]
    chunks += [(mask, layer) for layer in range(per_owner) for mask in order]
    weights = [t for t in range(1, members) if t != top]
    weights.sort(key=lambda t: (-(t & -t), t))
    lag = 3

    def relay(mask, layer):
        for place in range(1, columns):
            lowest = place & -place
            mp_copy(place ^ lowest, lowest, mask, layer).wait_recv()
            spread(place, lowest, mask, layer)

    for at in range(len(chunks) + lag):
        if at < len(chunks):
            mask, layer = chunks[at]
            if mask:
                dp_copy(mask, layer, me).wait_recv()
                spread(0, columns, mask, layer)
        if at >= members and at % 2 and weights:
            arrived = weights.pop(0)
            lowest = arrived & -arrived
            weight_copy(arrived ^ lowest, lowest).wait_recv()
            spread_weight(arrived, lowest)
        if at >= lag:
            relay(*chunks[at - lag])
    for arrived in weights:
        lowest = arrived & -arrived
        weight_copy(arrived ^ lowest, lowest).wait_recv()
        spread_weight(arrived, lowest)
    for copy in started:
        copy.wait_send()
    for copy in local:
        copy.wait()


def exchange(sent, weight, far_weight, members, columns):
    per_owner = sent.shape[1]
    anywhere = pl.BlockSpec(memory_space=pl.ANY)
    dma = pltpu.SemaphoreType.DMA
    return pl.pallas_call(
        functools.partial(exchange_kernel, members, columns, per_owner),
        out_shape=(
            jax.ShapeDtypeStruct((columns,) + sent.shape, sent.dtype),
            jax.ShapeDtypeStruct((members,) + weight.shape, weight.dtype),
        ),
        in_specs=[anywhere] * 3,
        out_specs=(anywhere, anywhere),
        scratch_shapes=[
            dma((3,)),
            dma((members, per_owner)),
            dma((members, per_owner)),
            dma((columns, members, per_owner)),
            dma((columns, members, per_owner)),
            dma((members,)),
            dma((members,)),
        ],
        compiler_params=pltpu.CompilerParams(collective_id=0, has_side_effects=True, vmem_limit_bytes=VMEM),
        cost_estimate=pl.CostEstimate(
            flops=0, bytes_accessed=60 * sent.size, transcendentals=0
        ),
    )(sent, weight, far_weight)


def project_kernel(columns, slots_ref, first_ref, second_ref, weight_ref, out_ref):
    total = None
    for column in range(columns):
        rows = jnp.concatenate([first_ref[column, 0], second_ref[column, 0]], axis=0)
        depth = rows.shape[1]
        part = jnp.dot(
            rows, weight_ref[column * depth:(column + 1) * depth, :],
            preferred_element_type=jnp.float32,
        )
        total = part if total is None else total + part
    out_ref[...] = total.astype(out_ref.dtype)


def project(slots, held, weight, kept):
    columns, total, _, depth = held.shape
    width = weight.shape[1]

    def picked(which):
        return pl.BlockSpec(
            (columns, 1, BLOCK, depth), lambda i, s: (0, s[1, 2 * i + which], 0, 0)
        )

    return pl.pallas_call(
        functools.partial(project_kernel, columns),
        out_shape=jax.ShapeDtypeStruct((kept * BLOCK, width), jnp.bfloat16),
        grid_spec=pltpu.PrefetchScalarGridSpec(
            num_scalar_prefetch=1,
            grid=(kept // 2,),
            in_specs=[
                picked(0),
                picked(1),
                pl.BlockSpec(weight.shape, lambda i, s: (0, 0)),
            ],
            out_specs=pl.BlockSpec((2 * BLOCK, width), lambda i, s: (i, 0)),
        ),
        compiler_params=pltpu.CompilerParams(vmem_limit_bytes=VMEM),
    )(slots, held, held, weight)


PIECES = 4
LAG = 5


def attend_block(block, queries_ref, keys_ref, values_ref, ids_ref, out_ref, owner, layer):
    repeat = queries_ref.shape[2] // HEAD_SIZE
    factor = math.log2(math.e) / math.sqrt(HEAD_SIZE)
    row_at = lax.broadcasted_iota(jnp.int32, (BLOCK, BLOCK), 0)
    col_at = lax.broadcasted_iota(jnp.int32, (BLOCK, BLOCK), 1)
    ones = jnp.ones((BLOCK, HEAD_SIZE), jnp.bfloat16)
    along = jnp.broadcast_to(ids_ref[block], (BLOCK, BLOCK))
    down = along.T
    bias = jnp.where((along == down) & (col_at <= row_at), 0.0, MASKED)
    value = jnp.where(down >= 0, values_ref[block].astype(jnp.float32), 0.0)
    value = jnp.concatenate([value.astype(jnp.bfloat16), ones], axis=1)
    key = keys_ref[block]
    query = queries_ref[block]
    query = jnp.concatenate(
        [query[:, h * HEAD_SIZE:(h + 1) * HEAD_SIZE] for h in range(repeat)], axis=0
    )
    scores = lax.dot_general(
        query, key, (((1,), (1,)), ((), ())), preferred_element_type=jnp.float32
    )
    weights = []
    for head in range(repeat):
        part = scores[head * BLOCK:(head + 1) * BLOCK] + bias
        highest = jnp.max(part, axis=1, keepdims=True)
        weights.append(jnp.exp2((part - highest) * factor).astype(jnp.bfloat16))
    summed = jnp.dot(
        jnp.concatenate(weights, axis=0), value, preferred_element_type=jnp.float32
    )
    summed = summed[:, :HEAD_SIZE] / summed[:, HEAD_SIZE:]
    for head in range(repeat):
        columns = slice(head * HEAD_SIZE, (head + 1) * HEAD_SIZE)
        out_ref[owner, layer * BLOCK:(layer + 1) * BLOCK, columns] = summed[
            head * BLOCK:(head + 1) * BLOCK
        ].astype(out_ref.dtype)


def differ(one, two, members):
    total, bit = 0, 1
    while bit < members:
        total = total + bit * ((one // bit + two // bit) % 2)
        bit *= 2
    return total


def merge(first, second, one=1, two=1):
    first, second, out = list(first), list(second), []
    while first or second:
        for _ in range(one):
            if first:
                out += first.pop(0)
        for _ in range(two):
            if second:
                out += second.pop(0)
    return out


def far_order(layers):
    order = [(m, l) for l in range(layers - 1) for m in (7, 5, 6, 4)]
    return order + [(m, l) for m in (5, 4, 7, 6) for l in (layers - 1, layers)]


def parts_of(mask, layers):
    return range(layers + 1 if mask > 3 else layers)


def after_sends(near_middle, layers):
    pieces = range(PIECES)
    block = range(layers)
    far = far_order(layers)
    near = [("a", m, l) for l in block for m in (2, 3)]
    out = []
    if near_middle:
        early = [("a", m, l) for m, l in far if m in (4, 5)]
        late = [("a", m, l) for m, l in far if m in (6, 7)]
        out += [("w", 6, p) for p in pieces]
        out += [("a", 1, l) for l in block]
        out += merge([[("w", 4, p)] for p in pieces], [[n] for n in near[:3]])
        out += near[3:] + early[:4]
        out += [("need", 1), ("need", 3), ("P", 0, 2)] + early[4:6] + [("P", 2, 2)] + early[6:]
        out += late[:1] + [("need", 7), ("R", 0, 2), ("R", 2, 2)] + late[1:2]
        out += [("P", 4, 1), ("P", 5, 1), ("R", 4, 2)] + late[2:4]
        out += [("need", 5), ("Q", 0, 2), ("Q", 2, 2), ("Q", 4, 2), ("keep", 0)]
        out += [("F", 0), ("F", 1)] + late[4:] + [("G", 6), ("G", 7)]
    else:
        early = [("a", m, l) for m, l in far if m in (6, 7)]
        late = [("a", m, l) for m, l in far if m in (4, 5)]
        weights = [("w", 6, p) for p in pieces]
        out += [("a", 1, l) for l in block]
        out += near
        out += merge([[("w", 4, p)] for p in pieces], [[e] for e in early[:3]])
        out += [("need", 1), ("need", 3), ("P", 0, 2)]
        out += [weights[0], late[0], early[3], ("P", 2, 2), late[1], weights[1]] + early[4:6]
        out += [("need", 5), ("R", 0, 2), late[2], weights[2]] + early[6:]
        out += [("R", 2, 2), ("P", 4, 1)]
        out += [weights[3], ("keep", 2), late[3], ("keep", 1), ("P", 5, 1)]
        out += late[4:6] + [("R", 4, 2)]
        out += [("need", 7), ("Q", 0, 2)] + late[6:] + [("Q", 2, 2), ("Q", 4, 2)]
        out += [("F", 0), ("F", 1), ("G", 6), ("G", 7)]
    return with_relays(out, near_middle, layers)


def units_of(near_middle):
    turn = 1 if near_middle else 3
    return [0, 1, 2, 3] + [u ^ turn for u in (4, 5, 6, 7)]


def with_relays(ops, near_middle, layers):
    units = units_of(near_middle)
    waiting = [(0, l) for l in range(layers)]
    out = []

    def settle(left):
        while len(waiting) > left:
            out.append(("x",) + waiting.pop(0))

    for op in ops:
        if op[0] == "keep":
            settle(op[1])
            continue
        if op[0] in ("P", "F", "G"):
            which = range(op[1], op[1] + op[2]) if op[0] == "P" else (6, 7)
            which = op[1:] if op[0] == "G" else which
            wanted = [(units[u], l) for u in which for l in parts_of(units[u], layers)]
            if op[0] != "P":
                first = op[1] if op[0] == "F" else layers - 1
                wanted = [w for w in wanted if min(w[1], layers - 1) == first]
            while any(w in waiting for w in wanted):
                settle(len(waiting) - 1)
            out.extend([("c", op[0], u) for u in which] if op[0] != "F" else [("c",) + op])
        out.append(op)
        if op[0] == "a":
            waiting.append(op[1:])
            settle(LAG)
    return out


def fused_kernel(
    members, columns, layers,
    queries_hbm, keys_hbm, values_hbm, ids_hbm, count_ref, weight_hbm,
    plan_ref, done_ref,
    queries_ref, keys_ref, values_ref, ids_ref, table_ref, own_ref, spot_ref,
    sent_ref, held_ref, full_ref, acc_ref,
    in_sem, spot_sem, send_n, recv_n, send_a, recv_a,
    send_x, recv_x, send_c, recv_c, send_w, recv_w, recv_y,
):
    me = lax.axis_index("dp")
    mine = lax.axis_index("mp")
    ring = me // 2
    middle = ((ring + 1) // 2) % 2
    inner = middle == 1
    outer = middle == 0
    half = ring // 2
    owned = weight_hbm.shape[0]
    piece = owned // PIECES
    depth = sent_ref.shape[2]
    reach = columns // 2 * depth

    barrier = pltpu.get_barrier_semaphore()
    for mask in range(1, members):
        pl.semaphore_signal(
            barrier, inc=1, device_id=(flip(me, mask), mine), device_id_type=MESH
        )
    for mask in (1, 2):
        pl.semaphore_signal(
            barrier, inc=1, device_id=(me, flip(mine, mask)), device_id_type=MESH
        )
    inputs = [
        pltpu.make_async_copy(ids_hbm, ids_ref, in_sem.at[0]),
        pltpu.make_async_copy(keys_hbm, keys_ref, in_sem.at[1]),
        pltpu.make_async_copy(values_hbm, values_ref, in_sem.at[2]),
        pltpu.make_async_copy(queries_hbm, queries_ref, in_sem.at[3]),
        pltpu.make_async_copy(
            weight_hbm,
            full_ref.at[pl.ds(pl.multiple_of(me * owned, owned), owned)],
            in_sem.at[4],
        ),
    ]
    for copy in inputs:
        copy.start()
    own_ref[...] = jnp.full(own_ref.shape, count_ref[0], jnp.int32)
    pl.semaphore_wait(barrier, members + 1)

    def remote(src, dst, send, recv, device):
        return pltpu.make_async_remote_copy(
            src_ref=src, dst_ref=dst, send_sem=send, recv_sem=recv,
            device_id=device, device_id_type=MESH,
        )

    def count_copy(mask):
        return remote(
            own_ref, table_ref.at[me], send_n, recv_n, (flip(me, mask), mine)
        )

    def rows_of(layer, mask=0):
        if mask > 3 and layer >= layers - 1:
            return pl.ds((layer + layers - 1) * (BLOCK // 2), BLOCK // 2)
        return pl.ds(layer * BLOCK, BLOCK)

    def block_copy(mask, layer):
        return remote(
            sent_ref.at[flip(me, mask), rows_of(layer, mask)],
            held_ref.at[mine, me, rows_of(layer, mask)],
            send_a, recv_a.at[mask, layer],
            (flip(me, mask), mine),
        )

    def x_copy(mask, layer):
        source = flip(me, mask)
        src = held_ref.at[mine, source, rows_of(layer, mask)]
        if mask == 0:
            src = sent_ref.at[me, rows_of(layer, mask)]
        return remote(
            src, held_ref.at[mine, source, rows_of(layer, mask)],
            send_x, recv_x.at[mask, layer],
            (me, flip(mine, 2)),
        )

    def core_sem(unit, layer):
        if unit < 6:
            return unit
        return 6 + layer if layer < layers - 1 else unit + layers - 1

    def core_copy(unit, mask, layer, far):
        source = flip(me, mask)
        column = flip(mine, 2 * far)
        src = held_ref.at[column, source, rows_of(layer, mask)]
        if mask == 0 and not far:
            src = sent_ref.at[me, rows_of(layer, mask)]
        return remote(
            src, held_ref.at[column, source, rows_of(layer, mask)],
            send_c, recv_c.at[core_sem(unit, layer)],
            (me, flip(mine, 1)),
        )

    def weight_copy(mask, to, part):
        first = pl.multiple_of(flip(me, mask) * owned + part * piece, piece)
        src = full_ref.at[pl.ds(first, piece)]
        if mask == 0:
            src = weight_hbm.at[pl.ds(pl.multiple_of(part * piece, piece), piece)]
        return remote(
            src, full_ref.at[pl.ds(first, piece)],
            send_w, recv_w.at[(mask ^ to) // 2, part] if to > 1 else recv_y.at[mask // 2],
            (flip(me, to), mine),
        )

    def landed(bytes_of, sem):
        pltpu.make_async_copy(bytes_of, bytes_of, sem).wait()

    def start(make, *where):
        make(*where).start()

    for mask in range(1, members):
        start(count_copy, mask)

    @pl.when(inner)
    def _():
        for part in range(PIECES):
            start(weight_copy, 0, 6, part)

    for part in range(PIECES):
        start(weight_copy, 0, 2, part)
    for part in range(PIECES // 2):
        start(weight_copy, 0, 1, part)

    table_ref[me] = own_ref[...]
    landed(table_ref.at[pl.ds(0, members - 1)], recv_n)
    lane = lax.broadcasted_iota(jnp.int32, own_ref.shape, 1)
    shift = members.bit_length() - 1
    begin = jnp.zeros(own_ref.shape, jnp.int32)
    first = jnp.zeros(own_ref.shape, jnp.int32)
    slots = jnp.zeros(own_ref.shape, jnp.int32)
    wanted = me + lane * members
    for member in range(members):
        count = table_ref[member]
        first = jnp.where(me == member, begin, first)
        within = wanted - begin
        holds = (within >= 0) & (within < count)
        slots = jnp.where(
            holds, member * layers + lax.shift_right_logical(within, shift), slots
        )
        begin = begin + count
    plan_ref[...] = slots
    table_ref[me] = first
    spot = pltpu.make_async_copy(table_ref.at[me], spot_ref, spot_sem)
    spot.start()
    for copy in inputs[:4]:
        copy.wait()
    spot.wait()
    turn = members * NB - spot_ref[0, 0]

    def attend_for(at):
        owner = differ(me, flip(at, 1), members)
        block = (owner + turn) & (members - 1)
        for layer in range(layers):
            attend_block(
                block + layer * members,
                queries_ref, keys_ref, values_ref, ids_ref, sent_ref, owner, layer,
            )

    @pl.loop(0, 2)
    def _(at):
        attend_for(at)

    for layer in range(layers):
        start(block_copy, 1, layer)
        start(x_copy, 0, layer)
        start(core_copy, 0, 0, layer, 0)
    for part in range(PIECES // 2, PIECES):
        start(weight_copy, 0, 1, part)
    held_ref[mine, me] = sent_ref[me]

    @pl.loop(2, 4)
    def _(at):
        attend_for(at)

    for layer in range(layers):
        for mask in (2, 3):
            start(block_copy, mask, layer)

    @pl.loop(4, 8)
    def _(at):
        attend_for(at)
        weight_copy(0, 2, at - 4).wait_recv()
        weight_copy(2, 1, at - 4).start()

        @pl.when(inner)
        def _():
            weight_copy(2, 6, at - 4).start()

    for mask, layer in far_order(layers):
        start(block_copy, mask, layer)
    inputs[4].wait()

    tile = 256
    width = full_ref.shape[1]

    def source_of(at):
        early = (at // 4 + 1) % 2
        far = flip(at, 1) * middle + flip(at, 3) * (1 - middle)
        return differ(me, early * at + (1 - early) * far, members)

    def part_of(column, source, rows, lanes):
        return jnp.dot(
            held_ref[column, source, rows, :],
            full_ref[pl.ds(pl.multiple_of(column * depth, depth), depth), lanes],
            preferred_element_type=jnp.float32,
        )

    every = pl.ds(0, layers * BLOCK)
    sooner = flip(ring, 3) * middle + flip(ring, 2) * (1 - middle)
    later = flip(ring, 2) * middle + flip(ring, 3) * (1 - middle)

    def near_product(at):
        source = source_of(at)
        for lane_at in range(0, width, tile):
            lanes = pl.ds(lane_at, tile)
            total = part_of(ring, source, every, lanes)
            acc_ref[at, :, lanes] = total + part_of(flip(ring, 1), source, every, lanes)

    def sooner_product(at):
        source = source_of(at)
        for lane_at in range(0, width, tile):
            lanes = pl.ds(lane_at, tile)
            acc_ref[at, :, lanes] += part_of(sooner, source, every, lanes)

    def later_product(at):
        source = source_of(at)
        for lane_at in range(0, width, tile):
            lanes = pl.ds(lane_at, tile)
            total = acc_ref[at, :, lanes] + part_of(later, source, every, lanes)
            done_ref[source, :, lanes] = total.astype(done_ref.dtype)

    def whole_product(layer):
        rows = rows_of(layer)
        one, two = source_of(6), source_of(7)
        for lane_at in range(0, width, tile):
            lanes = pl.ds(lane_at, tile)
            total = None
            for column in range(columns):
                part = jnp.dot(
                    jnp.concatenate(
                        [held_ref[column, one, rows, :], held_ref[column, two, rows, :]], axis=0
                    ),
                    full_ref[pl.ds(column * depth, depth), lanes],
                    preferred_element_type=jnp.float32,
                )
                total = part if total is None else total + part
            total = total.astype(done_ref.dtype)
            done_ref[one, rows, lanes] = total[:BLOCK]
            done_ref[two, rows, lanes] = total[BLOCK:]

    def last_product(at):
        source = source_of(at)
        rows = rows_of(layers - 1)
        for lane_at in range(0, width, tile):
            lanes = pl.ds(lane_at, tile)
            total = None
            for column in range(columns):
                part = part_of(column, source, rows, lanes)
                total = part if total is None else total + part
            done_ref[source, rows, lanes] = total.astype(done_ref.dtype)

    def product(kind, which, count=1):
        if kind == "F":
            whole_product(which)
        elif kind == "G":
            last_product(which)
        else:
            one = {"P": near_product, "R": sooner_product, "Q": later_product}[kind]
            pl.loop(which, which + count)(one)

    def step(op, near_middle):
        kind = op[0]
        units = units_of(near_middle)
        if kind == "a":
            block_copy(*op[1:]).wait_recv()
            start(x_copy, *op[1:])
            start(core_copy, units.index(op[1]), *op[1:], 0)
        elif kind == "x":
            x_copy(*op[1:]).wait_recv()
            start(core_copy, units.index(op[1]), *op[1:], 1)
        elif kind == "c" and op[1] == "P":
            landed(held_ref.at[pl.ds(0, 2), 0], recv_c.at[op[2]])
        elif kind == "c" and op[1] == "F":
            landed(held_ref.at[pl.ds(0, 4), 0, rows_of(op[2])], recv_c.at[6 + op[2]])
        elif kind == "c":
            landed(
                held_ref.at[pl.ds(0, 2), 0, rows_of(layers - 1)],
                recv_c.at[core_sem(op[2], layers - 1)],
            )
        elif kind == "need":
            first = pl.multiple_of(flip(me, op[1]) * owned, owned)
            landed(full_ref.at[pl.ds(first, owned)], recv_y.at[op[1] // 2])
        elif kind == "w":
            mask, part = op[1:]
            weight_copy(0, mask, part).wait_recv()
            if near_middle:
                start(weight_copy, mask, 2, part)
            start(weight_copy, mask, 1, part)

    plans = [after_sends(True, layers), after_sends(False, layers)]
    while plans[0]:
        stop = None
        for plan, near_middle, here in ((plans[0], True, inner), (plans[1], False, outer)):
            ops = []
            while plan and plan[0][0] not in ("P", "R", "Q", "F", "G"):
                ops.append(plan.pop(0))
            if ops:

                @pl.when(here)
                def _(ops=ops, near_middle=near_middle):
                    for op in ops:
                        step(op, near_middle)

            stop = plan.pop(0)
        product(*stop)

    landed(table_ref.at[pl.ds(0, members - 1)], send_n)
    landed(sent_ref.at[pl.ds(0, members - 1)], send_a)
    landed(sent_ref, send_x)
    landed(held_ref.at[pl.ds(0, 2)], send_c)

    @pl.when(inner)
    def _():
        landed(held_ref.at[pl.ds(0, 4), pl.ds(0, 3)], send_w)

    @pl.when(outer)
    def _():
        landed(full_ref.at[pl.ds(0, 5 * PIECES * piece)], send_w)


def fused(queries, keys, values, ids, live_counts, weight, members, columns, layers):
    anywhere = pl.BlockSpec(memory_space=pl.ANY)
    dma = pltpu.SemaphoreType.DMA
    rows = layers * BLOCK
    depth = queries.shape[2]
    width = weight.shape[1]
    low = jnp.bfloat16
    return pl.pallas_call(
        functools.partial(fused_kernel, members, columns, layers),
        out_shape=(
            pltpu.VMEM((8, 128), jnp.int32),
            pltpu.VMEM((members, rows, width), low),
        ),
        in_specs=[anywhere] * 4 + [pl.BlockSpec(memory_space=pltpu.SMEM), anywhere],
        out_specs=(pl.BlockSpec(memory_space=pltpu.VMEM),) * 2,
        scratch_shapes=[
            pltpu.VMEM(queries.shape, low),
            pltpu.VMEM(keys.shape, low),
            pltpu.VMEM(values.shape, low),
            pltpu.VMEM(ids.shape, jnp.int32),
            pltpu.VMEM((members, 8, 128), jnp.int32),
            pltpu.VMEM((8, 128), jnp.int32),
            pltpu.SMEM((8, 128), jnp.int32),
            pltpu.VMEM((members, rows, depth), low),
            pltpu.VMEM((columns, members, rows, depth), low),
            pltpu.VMEM((members * weight.shape[0], width), low),
            pltpu.VMEM((6, rows, width), jnp.float32),
            dma((5,)),
            dma,
            dma, dma,
            dma, dma((members, layers + 1)),
            dma, dma((members, layers + 1)),
            dma, dma((7 + layers,)),
            dma, dma((4, PIECES)), dma((4,)),
        ],
        compiler_params=pltpu.CompilerParams(
            collective_id=2, has_side_effects=True, vmem_limit_bytes=115 * 512 * 1024
        ),
    )(queries, keys, values, ids, live_counts, weight)


def order_kernel(slots_ref, products_ref, out_ref, sem):
    kept = out_ref.shape[0] // BLOCK
    copies = [
        pltpu.make_async_copy(
            products_ref.at[slots_ref[0, at]], out_ref.at[pl.ds(at * BLOCK, BLOCK)], sem.at[at]
        )
        for at in range(kept)
    ]
    for copy in copies:
        copy.start()
    for copy in copies:
        copy.wait()


def in_order(slots, products, kept):
    width = products.shape[2]
    return pl.pallas_call(
        order_kernel,
        out_shape=jax.ShapeDtypeStruct((kept * BLOCK, width), products.dtype),
        in_specs=[
            pl.BlockSpec(memory_space=pltpu.SMEM), pl.BlockSpec(memory_space=pltpu.VMEM)
        ],
        out_specs=pl.BlockSpec(memory_space=pl.ANY),
        scratch_shapes=[pltpu.SemaphoreType.DMA((kept,))],
        compiler_params=pltpu.CompilerParams(vmem_limit_bytes=16 * 1024 * 1024),
    )(slots, products)


def body(members, columns, queries, keys, values, doc_ids, live_counts, out_weight):
    per_owner = (NB + members - 1) // members
    kept = NB * 11 // 12
    half = members // 2
    if members == 8 and columns == 4:
        slots, products = fused(
            queries.reshape(NB, BLOCK, -1), keys.reshape(NB, BLOCK, -1),
            values.reshape(NB, BLOCK, -1), doc_ids.reshape(NB, 1, BLOCK),
            live_counts, out_weight,
            members, columns, per_owner,
        )
        products = products.reshape(members * per_owner, BLOCK, out_weight.shape[1])
        return in_order(slots, products, kept)
    plan = make_plan(live_counts, members, per_owner)
    plan, near_weight = lax.optimization_barrier((plan, out_weight))
    far_weight = lax.ppermute(
        near_weight, "dp", [(i, (i + half) % members) for i in range(members)]
    )
    sent = attend(
        plan, queries, keys, values, doc_ids.reshape(NB, BLOCK), members, per_owner
    )
    held, full = exchange(sent, out_weight, far_weight, members, columns)
    held = held.reshape(columns, members * per_owner, BLOCK, queries.shape[1])
    full = full.reshape(members * out_weight.shape[0], out_weight.shape[1])
    return project(plan, held, full, kept)


def solution(mesh):
    return jax.shard_map(
        functools.partial(body, mesh.shape["dp"], mesh.shape["mp"]),
        mesh=mesh,
        in_specs=(P("dp", "mp"), P("dp", "mp"), P("dp", "mp"), P("dp"), P("dp"), P("dp", "mp")),
        out_specs=P("dp", "mp"),
        check_vma=False,
    )
```
